8 devices in a mesh: data: 8 (over z, y, x, core).
Axes of the slice: x: 2, y: 2, z: 1, core: 2. Of those that a mesh axis runs over, the one named last changes fastest.
Arguments:
- tokens: bfloat16 [32768, 192], P('data')
- w_in: bfloat16 [192, 768], replicated
- w_out: bfloat16 [768, 192], replicated
- task_heads: bfloat16 [2, 192, 10], replicated
- labels: int32 [2, 32768], P(None, 'data')
- label_mask: int32 [2, 32768], P(None, 'data')
Outputs:
- output 1: float32 [2], replicated
- output 2: float32 [147456], P('data')
- output 3: float32 [147456], P('data')
All inputs are finite; a program needn't handle non-finite values.
Results may differ from the reference program's by a relative error of at most 0.00622191.
Values are sent between devices in bfloat16 or wider.
A program may use at most 1 GiB of HBM per device.

```python
import jax
import jax.numpy as jnp
from jax import lax

MODEL_DIM = 192
HIDDEN_DIM = 768
NUM_TASKS = 2
NUM_CLASSES = 10
TOK_DEV = 4096
GROUP_SIZE = 8
SOLVER_STEPS = 20


def draw_labels(rng_key):
    sub_keys = jax.random.split(rng_key, 7)
    tokens_total = TOK_DEV * GROUP_SIZE
    dev_class = jax.random.randint(sub_keys[0], (GROUP_SIZE, 1), 0, NUM_CLASSES)
    keep_draw = jax.random.randint(sub_keys[1], (GROUP_SIZE, TOK_DEV), 0, 4)
    free_class = jax.random.randint(sub_keys[2], (GROUP_SIZE, TOK_DEV), 0, NUM_CLASSES)
    common_class = jnp.where(keep_draw < 3, dev_class, free_class).reshape(tokens_total)
    noise_draw = jax.random.randint(sub_keys[3], (NUM_TASKS, tokens_total), 0, 4)
    task_class = jax.random.randint(sub_keys[4], (NUM_TASKS, tokens_total), 0, NUM_CLASSES)
    labels = jnp.where(noise_draw == 0, task_class, common_class[None, :]).astype(jnp.int32)
    mask_level = jax.random.randint(sub_keys[5], (NUM_TASKS, GROUP_SIZE, 1), 5, 100)
    mask_draw = jax.random.randint(sub_keys[6], (NUM_TASKS, GROUP_SIZE, TOK_DEV), 0, 100)
    label_mask = (mask_draw < mask_level).astype(jnp.int32).reshape(NUM_TASKS, tokens_total)
    return labels, label_mask


def setup_inputs(seed: int = 0) -> dict:
    rng_keys = jax.random.split(jax.random.key(seed), 6)
    tokens_total = TOK_DEV * GROUP_SIZE
    tokens = jax.random.normal(rng_keys[0], (tokens_total, MODEL_DIM), jnp.float32)
    w_in = jax.random.normal(rng_keys[1], (MODEL_DIM, HIDDEN_DIM), jnp.float32) * MODEL_DIM ** -0.5
    w_out = jax.random.normal(rng_keys[2], (HIDDEN_DIM, MODEL_DIM), jnp.float32) * HIDDEN_DIM ** -0.5
    shared_head = jax.random.normal(rng_keys[3], (MODEL_DIM, NUM_CLASSES), jnp.float32)
    own_head = jax.random.normal(rng_keys[4], (NUM_TASKS, MODEL_DIM, NUM_CLASSES), jnp.float32)
    head_sign = (1 - 2 * (jnp.arange(NUM_TASKS) % 2)).astype(jnp.float32)
    task_heads = (head_sign[:, None, None] * shared_head[None] + 0.6 * own_head) * (1.5 * MODEL_DIM ** -0.5)
    labels, label_mask = draw_labels(rng_keys[5])
    return {"tokens": tokens.astype(jnp.bfloat16), "w_in": w_in.astype(jnp.bfloat16), "w_out": w_out.astype(jnp.bfloat16), "task_heads": task_heads.astype(jnp.bfloat16), "labels": labels, "label_mask": label_mask}


def device_grads(x_loc, w_in, w_out, task_heads, lab_loc, mask_loc):
    pre_act = jnp.dot(x_loc, w_in, preferred_element_type=jnp.float32)
    act_out, gelu_slope = jax.jvp(jax.nn.gelu, (pre_act,), (jnp.ones_like(pre_act),))
    act_bf = act_out.astype(jnp.bfloat16)
    residual = x_loc.astype(jnp.float32) + jnp.dot(act_bf, w_out, preferred_element_type=jnp.float32)
    z_bf = residual.astype(jnp.bfloat16)
    heads_wide = task_heads.astype(jnp.float32)
    logits = jnp.einsum("bd,tdc->tbc", z_bf.astype(jnp.float32), heads_wide)
    soft_prob = jax.nn.softmax(logits, axis=-1)
    onehot = (lab_loc[:, :, None] == jnp.arange(NUM_CLASSES)[None, None, :]).astype(jnp.float32)
    d_logit = (mask_loc[:, :, None].astype(jnp.float32) * (soft_prob - onehot)).astype(jnp.bfloat16)
    d_resid = jnp.einsum("tbc,tdc->tbd", d_logit.astype(jnp.float32), heads_wide).astype(jnp.bfloat16)
    d_wide = d_resid.astype(jnp.float32)
    grad_w_out = jnp.einsum("bf,tbd->tfd", act_bf.astype(jnp.float32), d_wide)
    d_act = jnp.einsum("tbd,fd->tbf", d_wide, w_out.astype(jnp.float32))
    d_pre = (d_act * gelu_slope[None]).astype(jnp.bfloat16)
    grad_w_in = jnp.einsum("bd,tbf->tdf", x_loc.astype(jnp.float32), d_pre.astype(jnp.float32))
    return grad_w_in, grad_w_out


def solve_weights(gram_mat):
    step_scale = jnp.trace(gram_mat) / NUM_TASKS

    def solver_step(step_idx, weights):
        pull_vec = (gram_mat * weights[None, :]).sum(axis=1)
        raised = weights * jnp.exp(-pull_vec / step_scale)
        return raised / raised.sum()

    init_weights = jnp.full((NUM_TASKS,), 1.0 / NUM_TASKS, jnp.float32)
    return lax.fori_loop(0, SOLVER_STEPS, solver_step, init_weights)


def reference(tokens, w_in, w_out, task_heads, labels, label_mask):
    inv_count = 1.0 / jnp.maximum(label_mask.sum(axis=1), 1).astype(jnp.float32)
    tok_blocks = tokens.reshape(GROUP_SIZE, TOK_DEV, MODEL_DIM)
    lab_blocks = labels.reshape(NUM_TASKS, GROUP_SIZE, TOK_DEV).transpose(1, 0, 2)
    mask_blocks = label_mask.reshape(NUM_TASKS, GROUP_SIZE, TOK_DEV).transpose(1, 0, 2)
    flat_len = MODEL_DIM * HIDDEN_DIM

    def add_device(grad_sum, block_in):
        x_loc, lab_loc, mask_loc = block_in
        grad_w_in, grad_w_out = device_grads(x_loc, w_in, w_out, task_heads, lab_loc, mask_loc)
        flat_grad = jnp.concatenate([grad_w_in.reshape(NUM_TASKS, flat_len), grad_w_out.reshape(NUM_TASKS, flat_len)], axis=1)
        part_grad = (flat_grad * inv_count[:, None]).astype(jnp.bfloat16).astype(jnp.float32)
        return grad_sum + part_grad, None

    grad_sum, _ = lax.scan(add_device, jnp.zeros((NUM_TASKS, 2 * flat_len), jnp.float32), (tok_blocks, lab_blocks, mask_blocks))
    gram_mat = jnp.dot(grad_sum, grad_sum.T, preferred_element_type=jnp.float32)
    weights = solve_weights(gram_mat)
    combined = (weights[:, None] * grad_sum).sum(axis=0)
    return weights, combined[:flat_len], combined[flat_len:]
```

```python
import functools

import jax
import jax.numpy as jnp
from jax import lax
from jax.experimental import pallas as pl
from jax.experimental.pallas import tpu as pltpu
from jax.sharding import PartitionSpec as P

SOLVER_STEPS = 20
MESH = pl.DeviceIdType.MESH
F32 = jnp.float32
BF16 = jnp.bfloat16
LANES = 128
SLOT = 16
C0 = 0.7978845608028654
C1 = 0.044715

NT = (((1,), (1,)), ((), ()))
TN = (((0,), (0,)), ((), ()))


def peer_of(me, k):
    y, x, c = me // 4, (me // 2) % 2, me % 2
    return ((y + k // 4) % 2) * 4 + ((x + (k // 2) % 2) % 2) * 2 + (c + k % 2) % 2


def kernel(n, tb, fc, x_ref, w1_ref, w2_ref, h_ref, lab_ref, mask_ref,
           alpha_ref, gin_ref, gout_ref,
           a_s, slope_s, dz_s, dzt_s, xt_s, q_s, w2t_s, hc_s, hbt_s,
           send2, recv2, send1, recv1, cnt_send, cnt_recv, m_send, m_recv,
           flat0, flat1, ta_s, tr_s,
           send_sem, recv_sem):
    me = lax.axis_index("data")
    tokens, model = x_ref.shape
    hidden = w1_ref.shape[1]
    classes = h_ref.shape[2]
    nblk, nchunk = tokens // tb, hidden // fc
    rows_in, rows_out = model // n, hidden // n

    barrier = pltpu.get_barrier_semaphore()
    for k in range(1, n):
        pl.semaphore_signal(barrier, inc=1, device_id=(peer_of(me, k),), device_id_type=MESH)

    cnt = jnp.zeros((2, LANES), F32)
    for b in range(tokens // LANES):
        cnt += mask_ref[:, b * LANES:(b + 1) * LANES].astype(F32)
    cnt_send[0:2, :] = cnt
    cnt_send[2:8, :] = jnp.zeros((6, LANES), F32)

    w2t_s[...] = w2_ref[...].T
    pad = jnp.zeros((model, LANES - classes), F32)
    h0 = jnp.concatenate([h_ref[0].astype(F32), pad], axis=1)
    h1 = jnp.concatenate([h_ref[1].astype(F32), pad], axis=1)
    h1 = pltpu.roll(h1, SLOT, 1)
    hc_s[...] = (h0 + h1).T[:2 * SLOT].astype(BF16)
    hbt = jnp.concatenate([h0[:LANES], h1[:LANES], h0[LANES:], h1[LANES:]], axis=0)
    hbt_s[...] = hbt[:, :2 * SLOT].astype(BF16)

    def copies(slot, src_of, dst):
        out = []
        for k in range(1, n):
            peer = peer_of(me, k)
            out.append(pltpu.make_async_remote_copy(
                src_ref=src_of(peer), dst_ref=dst, send_sem=send_sem.at[slot, k],
                recv_sem=recv_sem.at[slot, k], device_id=(peer,), device_id_type=MESH))
        return out

    cnt_copies = copies(0, lambda peer: cnt_send, cnt_recv.at[me])

    def forward(i, carry):
        tok = pl.ds(pl.multiple_of(i * tb, tb), tb)
        x_b = x_ref[tok, :]
        xt_s[:, tok] = x_b.T
        for c in range(nchunk):
            f = slice(c * fc, (c + 1) * fc)
            p = jnp.dot(x_b, w1_ref[:, f], preferred_element_type=F32)
            p2 = p * p
            t = jnp.tanh(p * (C0 + (C0 * C1) * p2))
            h = 0.5 + 0.5 * t
            a = p * h
            a_s[tok, f] = a.astype(BF16)
            slope_s[tok, f] = h + (a * (1.0 - h)) * (2 * C0 + (6 * C0 * C1) * p2)
        z = x_b.astype(F32) + jnp.dot(a_s[tok, :], w2_ref[...], preferred_element_type=F32)
        logits = lax.dot_general(hc_s[...], z.astype(BF16), NT, preferred_element_type=F32)
        e_all = []
        for t in range(2):
            lg = logits[t * SLOT:(t + 1) * SLOT]
            cls = lax.broadcasted_iota(jnp.int32, (SLOT, tb), 0)
            lg = jnp.where(cls < classes, lg, -jnp.inf)
            ex = jnp.exp(lg - lg.max(axis=0, keepdims=True))
            prob = ex * (1.0 / ex.sum(axis=0, keepdims=True))
            hot = (cls == lab_ref[t:t + 1, tok]).astype(F32)
            e = (mask_ref[t:t + 1, tok].astype(F32) * (prob - hot)).astype(BF16)
            e_all.append(e)
            dz_s[t, tok, :] = lax.dot_general(
                e, hc_s[t * SLOT:(t + 1) * SLOT, :], TN, preferred_element_type=F32).astype(BF16)
        e_cat = jnp.concatenate(e_all, axis=0)
        dzt_s[:, tok] = jnp.dot(hbt_s[...], e_cat, preferred_element_type=F32).astype(BF16)

        @pl.when(i == 1)
        def _():
            pl.semaphore_wait(barrier, n - 1)
            for c in cnt_copies:
                c.start()

        return carry

    lax.fori_loop(0, nblk, forward, 0)

    for c in cnt_copies:
        c.wait()
    cnt_recv[me] = cnt_send[...]
    tot = cnt_recv[0]
    for j in range(1, n):
        tot += cnt_recv[j]
    inv = 1.0 / jnp.maximum(tot.sum(axis=1, keepdims=True), 1.0)
    inv0, inv1 = inv[0:1], inv[1:2]

    for c in range(nchunk):
        f = slice(c * fc, (c + 1) * fc)
        d = jnp.dot(dzt_s[...], a_s[:, f], preferred_element_type=F32)
        tail = 2 * LANES + (model - LANES)
        d = jnp.concatenate([d[:LANES] * inv0, d[LANES:2 * LANES] * inv1,
                             d[2 * LANES:tail] * inv0, d[tail:] * inv1], axis=0)
        send2[f, :] = d.T.astype(BF16)

    def rows_of(peer):
        return send2.at[pl.ds(pl.multiple_of(peer * rows_out, rows_out), rows_out)]

    out_copies = copies(1, rows_of, recv2.at[me])
    for c in out_copies:
        c.start()

    in_copies = []
    for c in range(nchunk):
        f = slice(c * fc, (c + 1) * fc)

        def backward(i, carry):
            tok = pl.ds(pl.multiple_of(i * tb, tb), tb)
            sl = slope_s[tok, f]
            for t in range(2):
                da = jnp.dot(dz_s[t, tok, :], w2t_s[:, f], preferred_element_type=F32)
                q_s[t, tok, :] = (da * sl).astype(BF16)
            return carry

        lax.fori_loop(0, nblk, backward, 0)
        d0 = jnp.dot(xt_s[...], q_s[0], preferred_element_type=F32) * inv0
        d1 = jnp.dot(xt_s[...], q_s[1], preferred_element_type=F32) * inv1
        for j in range(n):
            r = slice(j * rows_in, (j + 1) * rows_in)
            send1[c, j] = jnp.concatenate([d0[r], d1[r]], axis=0).astype(BF16)
        now = copies(2 + c, lambda peer: send1.at[c, peer], recv1.at[c, me])
        for cp in now:
            cp.start()
        in_copies.append(now)

    for cp in out_copies:
        cp.wait()
    recv2[me] = send2[pl.ds(pl.multiple_of(me * rows_out, rows_out), rows_out), :]
    g2 = recv2[0].astype(F32)
    for j in range(1, n):
        g2 += recv2[j].astype(F32)
    t0, t1, r = g2[:, :LANES], g2[:, LANES:2 * LANES], g2[:, 2 * LANES:]
    r_sw = pltpu.roll(r, LANES // 2, 1)
    low = lax.broadcasted_iota(jnp.int32, (1, LANES), 1) < LANES // 2

    def fold(v):
        s = v[0:8]
        for b in range(1, v.shape[0] // 8):
            s += v[8 * b:8 * b + 8]
        return s

    zero = jnp.zeros((8, LANES), F32)
    rr = fold(r * r)
    m00 = fold(t0 * t0) + jnp.where(low, rr, zero)
    m11 = fold(t1 * t1) + jnp.where(low, zero, rr)
    m01 = fold(t0 * t1) + jnp.where(low, fold(r * r_sw), zero)

    half = rows_out // 2
    for t, flat in ((0, flat0), (1, flat1)):
        ta_s[...] = t0 if t == 0 else t1
        tr_s[...] = r if t == 0 else r_sw
        a_e, a_o = ta_s[pl.ds(0, half, stride=2), :], ta_s[pl.ds(1, half, stride=2), :]
        r_e, r_o = tr_s[pl.ds(0, half, stride=2), :], tr_s[pl.ds(1, half, stride=2), :]
        a_w = pltpu.roll(a_o, LANES // 2, 1)
        flat[1, pl.ds(0, half, stride=3), :] = a_e
        flat[1, pl.ds(1, half, stride=3), :] = jnp.where(low, r_e, a_w)
        flat[1, pl.ds(2, half, stride=3), :] = jnp.where(low, a_w, pltpu.roll(r_o, LANES // 2, 1))

    wide = hidden // LANES
    for c in range(nchunk):
        for cp in in_copies[c]:
            cp.wait()
        recv1[c, me] = send1[c, me]
        g1 = recv1[c, 0].astype(F32)
        for j in range(1, n):
            g1 += recv1[c, j].astype(F32)
        for b in range(fc // LANES):
            u = g1[:rows_in, b * LANES:(b + 1) * LANES]
            v = g1[rows_in:, b * LANES:(b + 1) * LANES]
            m00 += fold(u * u)
            m11 += fold(v * v)
            m01 += fold(u * v)
            flat0[0, pl.ds(c * (fc // LANES) + b, rows_in, stride=wide), :] = u
            flat1[0, pl.ds(c * (fc // LANES) + b, rows_in, stride=wide), :] = v

    row = lax.broadcasted_iota(jnp.int32, (8, LANES), 0)
    m_send[...] = jnp.where(row == 0, m00.sum(axis=0, keepdims=True),
                            jnp.where(row == 1, m01.sum(axis=0, keepdims=True),
                                      jnp.where(row == 2, m11.sum(axis=0, keepdims=True), zero)))
    m_copies = copies(2 + nchunk, lambda peer: m_send, m_recv.at[me])
    for cp in m_copies:
        cp.start()
    for cp in m_copies:
        cp.wait()
    m_recv[me] = m_send[...]
    gram = m_recv[0]
    for j in range(1, n):
        gram += m_recv[j]
    gram = jnp.broadcast_to(gram.sum(axis=1, keepdims=True), (8, LANES))
    g00, g01, g11 = gram[0:1], gram[1:2], gram[2:3]
    scale = 1.0 / ((g00 + g11) * 0.5)
    b0, b1 = (g00 - g01) * scale, (g01 - g11) * scale
    gap = jnp.zeros((1, LANES), F32)
    a0 = jnp.full((1, LANES), 0.5, F32)
    a1 = a0
    for _ in range(SOLVER_STEPS):
        gap = gap + (b0 * a0 + b1 * a1)
        ratio = jnp.exp(gap)
        a0 = 1.0 / (1.0 + ratio)
        a1 = ratio * a0
    lane = lax.broadcasted_iota(jnp.int32, (1, LANES), 1)
    alpha_ref[...] = jnp.where(lane == 0, a0, a1)
    gin_ref[...] = a0 * flat0[0] + a1 * flat1[0]
    gout_ref[...] = a0 * flat0[1] + a1 * flat1[1]


def solution(mesh):
    n = mesh.shape["data"]
    tb, fc = 512, 256

    def local_step(x_loc, w_in, w_out, task_heads, lab_loc, mask_loc):
        tokens, model = x_loc.shape
        hidden = w_in.shape[1]
        nchunk = hidden // fc
        piece = model * hidden // n // LANES
        rows_in, rows_out = model // n, hidden // n
        vmem = pl.BlockSpec(memory_space=pltpu.VMEM)
        alpha, g_in, g_out = pl.pallas_call(
            functools.partial(kernel, n, tb, fc),
            out_shape=(jax.ShapeDtypeStruct((1, LANES), F32),
                       jax.ShapeDtypeStruct((piece, LANES), F32),
                       jax.ShapeDtypeStruct((piece, LANES), F32)),
            in_specs=[vmem] * 6,
            out_specs=(vmem, vmem, vmem),
            scratch_shapes=[
                pltpu.VMEM((tokens, hidden), BF16),
                pltpu.VMEM((tokens, hidden), F32),
                pltpu.VMEM((2, tokens, model), BF16),
                pltpu.VMEM((2 * model, tokens), BF16),
                pltpu.VMEM((model, tokens), BF16),
                pltpu.VMEM((2, tokens, fc), BF16),
                pltpu.VMEM((model, hidden), BF16),
                pltpu.VMEM((2 * SLOT, model), BF16),
                pltpu.VMEM((2 * model, 2 * SLOT), BF16),
                pltpu.VMEM((hidden, 2 * model), BF16),
                pltpu.VMEM((n, rows_out, 2 * model), BF16),
                pltpu.VMEM((nchunk, n, 2 * rows_in, fc), BF16),
                pltpu.VMEM((nchunk, n, 2 * rows_in, fc), BF16),
                pltpu.VMEM((8, LANES), F32),
                pltpu.VMEM((n, 8, LANES), F32),
                pltpu.VMEM((8, LANES), F32),
                pltpu.VMEM((n, 8, LANES), F32),
                pltpu.VMEM((2, piece, LANES), F32),
                pltpu.VMEM((2, piece, LANES), F32),
                pltpu.VMEM((rows_out, LANES), F32),
                pltpu.VMEM((rows_out, LANES), F32),
                pltpu.SemaphoreType.DMA((3 + nchunk, n)),
                pltpu.SemaphoreType.DMA((3 + nchunk, n)),
            ],
            compiler_params=pltpu.CompilerParams(
                collective_id=0, has_side_effects=True, vmem_limit_bytes=60 * 1024 * 1024),
        )(x_loc, w_in, w_out, task_heads, lab_loc, mask_loc)
        return alpha[0, :2], g_in.reshape(-1), g_out.reshape(-1)

    return jax.shard_map(local_step, mesh=mesh, in_specs=(P("data", None), P(), P(), P(), P(None, "data"), P(None, "data")), out_specs=(P(), P("data"), P("data")), check_vma=False)
```

```python
import functools

import jax
import jax.numpy as jnp
from jax import lax
from jax.experimental import pallas as pl
from jax.experimental.pallas import tpu as pltpu
from jax.sharding import PartitionSpec as P

SOLVER_STEPS = 20
MESH = pl.DeviceIdType.MESH
F32 = jnp.float32
BF16 = jnp.bfloat16
LANES = 128
SLOT = 16
C0 = 0.7978845608028654
C1 = 0.044715

NT = (((1,), (1,)), ((), ()))
TN = (((0,), (0,)), ((), ()))


def peer_of(me, k):
    y, x, c = me // 4, (me // 2) % 2, me % 2
    return ((y + k // 4) % 2) * 4 + ((x + (k // 2) % 2) % 2) * 2 + (c + k % 2) % 2


def kernel(n, tb, fc, xt_ref, w1_ref, w2t_ref, h_ref, lab_ref, mask_ref,
           flat0, flat1, gram_ref,
           a_s, slope_s, dz_s, dzt_s, z_s, q_s, w2_s, hc_s, hbt_s,
           send2, recv2, send1, recv1, cnt_send, cnt_recv, m_send, m_recv,
           ta_s, tr_s,
           send_sem, recv_sem):
    me = lax.axis_index("data")
    model, tokens = xt_ref.shape
    hidden = w1_ref.shape[1]
    classes = h_ref.shape[0]
    nblk, nchunk = tokens // tb, hidden // fc
    rows_in, rows_out = model // n, hidden // n

    barrier = pltpu.get_barrier_semaphore()
    for k in range(1, n):
        pl.semaphore_signal(barrier, inc=1, device_id=(peer_of(me, k),), device_id_type=MESH)

    cnt = jnp.zeros((2, LANES), F32)
    for b in range(tokens // LANES):
        cnt += mask_ref[:, b * LANES:(b + 1) * LANES].astype(F32)
    cnt_send[0:2, :] = cnt
    cnt_send[2:8, :] = jnp.zeros((6, LANES), F32)

    w2_s[...] = w2t_ref[...].T
    heads = h_ref[...].astype(F32)
    gap = jnp.zeros((SLOT - classes, model), F32)
    hc = jnp.concatenate([heads[:, 0], gap, heads[:, 1], gap], axis=0)
    hc_s[...] = hc.astype(BF16)
    full = jnp.concatenate([hc, jnp.zeros((LANES - 2 * SLOT, model), F32)], axis=0).T
    lane = lax.broadcasted_iota(jnp.int32, (1, LANES), 1)
    h0 = jnp.where(lane < SLOT, full, 0.0)
    h1 = jnp.where(lane < SLOT, 0.0, full)
    hbt = jnp.concatenate([h0[:LANES], h1[:LANES], h0[LANES:], h1[LANES:]], axis=0)
    hbt_s[...] = hbt[:, :2 * SLOT].astype(BF16)

    def copies(slot, src_of, dst):
        out = []
        for k in range(1, n):
            peer = peer_of(me, k)
            out.append(pltpu.make_async_remote_copy(
                src_ref=src_of(peer), dst_ref=dst, send_sem=send_sem.at[slot, k],
                recv_sem=recv_sem.at[slot, k], device_id=(peer,), device_id_type=MESH))
        return out

    cnt_copies = copies(0, lambda peer: cnt_send, cnt_recv.at[me])

    def block(i):
        return pl.ds(pl.multiple_of(i * tb, tb), tb)

    def errors(i, slot):
        tok = block(i)
        logits = lax.dot_general(hc_s[...], z_s[slot], NT, preferred_element_type=F32)
        e_all = []
        for t in range(2):
            lg = logits[t * SLOT:(t + 1) * SLOT]
            cls = lax.broadcasted_iota(jnp.int32, (SLOT, tb), 0)
            lg = jnp.where(cls < classes, lg, -jnp.inf)
            ex = jnp.exp(lg - lg.max(axis=0, keepdims=True))
            prob = ex * (1.0 / ex.sum(axis=0, keepdims=True))
            hot = (cls == lab_ref[t:t + 1, tok]).astype(F32)
            e = (mask_ref[t:t + 1, tok].astype(F32) * (prob - hot)).astype(BF16)
            e_all.append(e)
            dz_s[t, tok, :] = lax.dot_general(
                e, hc_s[t * SLOT:(t + 1) * SLOT, :], TN, preferred_element_type=F32).astype(BF16)
        e_cat = jnp.concatenate(e_all, axis=0)
        dzt_s[:, tok] = jnp.dot(hbt_s[...], e_cat, preferred_element_type=F32).astype(BF16)

    def trunk(i, slot):
        tok = block(i)
        x_b = xt_ref[:, tok].T
        for c in range(nchunk):
            f = slice(c * fc, (c + 1) * fc)
            p = jnp.dot(x_b, w1_ref[:, f], preferred_element_type=F32)
            p2 = p * p
            t = jnp.tanh(p * (C0 + (C0 * C1) * p2))
            h = 0.5 + 0.5 * t
            a = p * h
            a_s[tok, f] = a.astype(BF16)
            slope_s[tok, f] = h + (a * (1.0 - h)) * (2 * C0 + (6 * C0 * C1) * p2)
        z = x_b.astype(F32) + jnp.dot(a_s[tok, :], w2_s[...], preferred_element_type=F32)
        z_s[slot] = z.astype(BF16)

    trunk(0, 0)

    def forward(i, carry):
        errors(i - 1, (i - 1) % 2)
        trunk(i, i % 2)

        @pl.when(i == 1)
        def _():
            pl.semaphore_wait(barrier, n - 1)
            for c in cnt_copies:
                c.start()

        return carry

    lax.fori_loop(1, nblk, forward, 0)
    errors(nblk - 1, (nblk - 1) % 2)

    for c in cnt_copies:
        c.wait()
    cnt_recv[me] = cnt_send[...]
    tot = cnt_recv[0]
    for j in range(1, n):
        tot += cnt_recv[j]
    inv = 1.0 / jnp.maximum(tot.sum(axis=1, keepdims=True), 1.0)
    inv0, inv1 = inv[0:1], inv[1:2]

    for c in range(nchunk):
        f = slice(c * fc, (c + 1) * fc)
        d = jnp.dot(dzt_s[...], a_s[:, f], preferred_element_type=F32)
        tail = 2 * LANES + (model - LANES)
        d = jnp.concatenate([d[:LANES] * inv0, d[LANES:2 * LANES] * inv1,
                             d[2 * LANES:tail] * inv0, d[tail:] * inv1], axis=0)
        send2[f, :] = d.T.astype(BF16)

    def rows_of(peer):
        return send2.at[pl.ds(pl.multiple_of(peer * rows_out, rows_out), rows_out)]

    out_copies = copies(1, rows_of, recv2.at[me])
    for c in out_copies:
        c.start()

    in_copies = []
    for c in range(nchunk):
        f = slice(c * fc, (c + 1) * fc)

        for i in range(nblk):
            tok = slice(i * tb, (i + 1) * tb)
            sl = slope_s[tok, f]
            for t in range(2):
                da = jnp.dot(dz_s[t, tok, :], w2t_ref[:, f], preferred_element_type=F32)
                q_s[t, tok, :] = (da * sl).astype(BF16)
        d0 = jnp.dot(xt_ref[...], q_s[0], preferred_element_type=F32) * inv0
        d1 = jnp.dot(xt_ref[...], q_s[1], preferred_element_type=F32) * inv1
        for j in range(n):
            r = slice(j * rows_in, (j + 1) * rows_in)
            send1[c, j] = jnp.concatenate([d0[r], d1[r]], axis=0).astype(BF16)
        now = copies(2 + c, lambda peer: send1.at[c, peer], recv1.at[c, me])
        for cp in now:
            cp.start()
        in_copies.append(now)

    for cp in out_copies:
        cp.wait()
    recv2[me] = send2[pl.ds(pl.multiple_of(me * rows_out, rows_out), rows_out), :]
    g2 = recv2[0].astype(F32)
    for j in range(1, n):
        g2 += recv2[j].astype(F32)
    t0, t1, r = g2[:, :LANES], g2[:, LANES:2 * LANES], g2[:, 2 * LANES:]
    r_sw = pltpu.roll(r, LANES // 2, 1)
    low = lax.broadcasted_iota(jnp.int32, (1, LANES), 1) < LANES // 2

    def fold(v):
        s = v[0:8]
        for b in range(1, v.shape[0] // 8):
            s += v[8 * b:8 * b + 8]
        return s

    zero = jnp.zeros((8, LANES), F32)
    rr = fold(r * r)
    m00 = fold(t0 * t0) + jnp.where(low, rr, zero)
    m11 = fold(t1 * t1) + jnp.where(low, zero, rr)
    m01 = fold(t0 * t1) + jnp.where(low, fold(r * r_sw), zero)

    half = rows_out // 2
    for t, flat in ((0, flat0), (1, flat1)):
        ta_s[...] = t0 if t == 0 else t1
        tr_s[...] = r if t == 0 else r_sw
        a_e, a_o = ta_s[pl.ds(0, half, stride=2), :], ta_s[pl.ds(1, half, stride=2), :]
        r_e, r_o = tr_s[pl.ds(0, half, stride=2), :], tr_s[pl.ds(1, half, stride=2), :]
        a_w = pltpu.roll(a_o, LANES // 2, 1)
        flat[1, pl.ds(0, half, stride=3), :] = a_e
        flat[1, pl.ds(1, half, stride=3), :] = jnp.where(low, r_e, a_w)
        flat[1, pl.ds(2, half, stride=3), :] = jnp.where(low, a_w, pltpu.roll(r_o, LANES // 2, 1))

    wide = hidden // LANES
    for c in range(nchunk):
        for cp in in_copies[c]:
            cp.wait()
        recv1[c, me] = send1[c, me]
        g1 = recv1[c, 0].astype(F32)
        for j in range(1, n):
            g1 += recv1[c, j].astype(F32)
        for b in range(fc // LANES):
            u = g1[:rows_in, b * LANES:(b + 1) * LANES]
            v = g1[rows_in:, b * LANES:(b + 1) * LANES]
            m00 += fold(u * u)
            m11 += fold(v * v)
            m01 += fold(u * v)
            flat0[0, pl.ds(c * (fc // LANES) + b, rows_in, stride=wide), :] = u
            flat1[0, pl.ds(c * (fc // LANES) + b, rows_in, stride=wide), :] = v

    row = lax.broadcasted_iota(jnp.int32, (8, LANES), 0)
    m_send[...] = jnp.where(row == 0, m00.sum(axis=0, keepdims=True),
                            jnp.where(row == 1, m01.sum(axis=0, keepdims=True),
                                      jnp.where(row == 2, m11.sum(axis=0, keepdims=True), zero)))
    m_copies = copies(2 + nchunk, lambda peer: m_send, m_recv.at[me])
    for cp in m_copies:
        cp.start()
    for cp in m_copies:
        cp.wait()
    m_recv[me] = m_send[...]
    gram = m_recv[0]
    for j in range(1, n):
        gram += m_recv[j]
    gram_ref[...] = gram


def finish(u0_ref, u1_ref, gram_ref, alpha_ref, gin_ref, gout_ref):
    gram = jnp.broadcast_to(gram_ref[...].sum(axis=1, keepdims=True), (8, LANES))
    g00, g01, g11 = gram[0:1], gram[1:2], gram[2:3]
    scale = 1.0 / ((g00 + g11) * 0.5)
    b0, b1 = (g00 - g01) * scale, (g01 - g11) * scale
    gap = jnp.zeros((1, LANES), F32)
    a0 = jnp.full((1, LANES), 0.5, F32)
    a1 = a0
    for _ in range(SOLVER_STEPS):
        gap = gap + (b0 * a0 + b1 * a1)
        ratio = jnp.exp(gap)
        a0 = 1.0 / (1.0 + ratio)
        a1 = ratio * a0
    alpha_ref[0] = a0[0, 0]
    alpha_ref[1] = a1[0, 0]
    gin_ref[...] = a0 * u0_ref[0] + a1 * u1_ref[0]
    gout_ref[...] = a0 * u0_ref[1] + a1 * u1_ref[1]


def solution(mesh):
    n = mesh.shape["data"]
    tb, fc = 512, 256

    def local_step(x_loc, w_in, w_out, task_heads, lab_loc, mask_loc):
        tokens, model = x_loc.shape
        hidden = w_in.shape[1]
        nchunk = hidden // fc
        piece = model * hidden // n // LANES
        rows_in, rows_out = model // n, hidden // n
        vmem = pl.BlockSpec(memory_space=pltpu.VMEM)
        u0, u1, gram = pl.pallas_call(
            functools.partial(kernel, n, tb, fc),
            out_shape=(jax.ShapeDtypeStruct((2, piece, LANES), F32),
                       jax.ShapeDtypeStruct((2, piece, LANES), F32),
                       jax.ShapeDtypeStruct((8, LANES), F32)),
            in_specs=[vmem] * 6,
            out_specs=(vmem, vmem, vmem),
            scratch_shapes=[
                pltpu.VMEM((tokens, hidden), BF16),
                pltpu.VMEM((tokens, hidden), F32),
                pltpu.VMEM((2, tokens, model), BF16),
                pltpu.VMEM((2 * model, tokens), BF16),
                pltpu.VMEM((2, tb, model), BF16),
                pltpu.VMEM((2, tokens, fc), BF16),
                pltpu.VMEM((hidden, model), BF16),
                pltpu.VMEM((2 * SLOT, model), BF16),
                pltpu.VMEM((2 * model, 2 * SLOT), BF16),
                pltpu.VMEM((hidden, 2 * model), BF16),
                pltpu.VMEM((n, rows_out, 2 * model), BF16),
                pltpu.VMEM((nchunk, n, 2 * rows_in, fc), BF16),
                pltpu.VMEM((nchunk, n, 2 * rows_in, fc), BF16),
                pltpu.VMEM((8, LANES), F32),
                pltpu.VMEM((n, 8, LANES), F32),
                pltpu.VMEM((8, LANES), F32),
                pltpu.VMEM((n, 8, LANES), F32),
                pltpu.VMEM((rows_out, LANES), F32),
                pltpu.VMEM((rows_out, LANES), F32),
                pltpu.SemaphoreType.DMA((3 + nchunk, n)),
                pltpu.SemaphoreType.DMA((3 + nchunk, n)),
            ],
            compiler_params=pltpu.CompilerParams(
                collective_id=0, has_side_effects=True, vmem_limit_bytes=60 * 1024 * 1024),
        )(x_loc.T, w_in, w_out.T, jnp.transpose(task_heads, (2, 0, 1)), lab_loc, mask_loc)
        alpha, g_in, g_out = pl.pallas_call(
            finish,
            out_shape=(jax.ShapeDtypeStruct((2,), F32),
                       jax.ShapeDtypeStruct((piece, LANES), F32),
                       jax.ShapeDtypeStruct((piece, LANES), F32)),
            in_specs=[vmem] * 3,
            out_specs=(pl.BlockSpec(memory_space=pltpu.SMEM), vmem, vmem),
        )(u0, u1, gram)
        return alpha, g_in.reshape(-1), g_out.reshape(-1)

    return jax.shard_map(local_step, mesh=mesh, in_specs=(P("data", None), P(), P(), P(), P(None, "data"), P(None, "data")), out_specs=(P(), P("data"), P("data")), check_vma=False)
```

```python
import functools

import jax
import jax.numpy as jnp
from jax import lax
from jax.experimental import pallas as pl
from jax.experimental.pallas import tpu as pltpu
from jax.sharding import PartitionSpec as P

SOLVER_STEPS = 20
MESH = pl.DeviceIdType.MESH
F32 = jnp.float32
BF16 = jnp.bfloat16
LANES = 128
SLOT = 16
C0 = 0.7978845608028654
C1 = 0.044715

NT = (((1,), (1,)), ((), ()))
TN = (((0,), (0,)), ((), ()))


def peer_of(me, k):
    y, x, c = me // 4, (me // 2) % 2, me % 2
    return ((y + k // 4) % 2) * 4 + ((x + (k // 2) % 2) % 2) * 2 + (c + k % 2) % 2


def kernel(n, tb, rp, fc, xt_ref, w1_ref, w2t_ref, h_ref, lab_ref, mask_ref,
           flat0, flat1, gram_ref,
           x_s, sl_s, a_s, p_s, e_s, dz_s, dzt_s, z_s, acc_s, q_s, w2_s, hc_s, hbt_s,
           send2, recv2, send1, recv1, cnt_send, cnt_recv, m_send, m_recv,
           ta_s, tr_s,
           send_sem, recv_sem):
    me = lax.axis_index("data")
    model, tokens = xt_ref.shape
    hidden = w1_ref.shape[1]
    classes = h_ref.shape[0]
    nblk, nchunk = tokens // tb, hidden // fc
    rows_in, rows_out = model // n, hidden // n

    barrier = pltpu.get_barrier_semaphore()
    for k in range(1, n):
        pl.semaphore_signal(barrier, inc=1, device_id=(peer_of(me, k),), device_id_type=MESH)

    cnt = jnp.zeros((2, LANES), F32)
    for b in range(tokens // LANES):
        cnt += mask_ref[:, b * LANES:(b + 1) * LANES].astype(F32)
    cnt_send[0:2, :] = cnt
    cnt_send[2:8, :] = jnp.zeros((6, LANES), F32)

    w2_s[...] = w2t_ref[...].T
    heads = h_ref[...].astype(F32)
    gap = jnp.zeros((SLOT - classes, model), F32)
    hc = jnp.concatenate([heads[:, 0], gap, heads[:, 1], gap], axis=0)
    hc_s[...] = hc.astype(BF16)
    full = jnp.concatenate([hc, jnp.zeros((LANES - 2 * SLOT, model), F32)], axis=0).T
    lane = lax.broadcasted_iota(jnp.int32, (1, LANES), 1)
    h0 = jnp.where(lane < SLOT, full, 0.0)
    h1 = jnp.where(lane < SLOT, 0.0, full)
    hbt = jnp.concatenate([h0[:LANES], h1[:LANES], h0[LANES:], h1[LANES:]], axis=0)
    hbt_s[...] = hbt[:, :2 * SLOT].astype(BF16)

    def copies(slot, src_of, dst):
        out = []
        for k in range(1, n):
            peer = peer_of(me, k)
            out.append(pltpu.make_async_remote_copy(
                src_ref=src_of(peer), dst_ref=dst, send_sem=send_sem.at[slot, k],
                recv_sem=recv_sem.at[slot, k], device_id=(peer,), device_id_type=MESH))
        return out

    cnt_copies = copies(0, lambda peer: cnt_send, cnt_recv.at[me])

    def block(i):
        return slice(i * tb, (i + 1) * tb)

    def chunk(c):
        return pl.ds(pl.multiple_of(c * fc, fc), fc) if not isinstance(c, int) else slice(c * fc, (c + 1) * fc)

    def enter(i):
        if i < nblk:
            x_s[block(i), :] = xt_ref[:, block(i)].T

    def project(i, c):
        if i < nblk:
            p_s[block(i), chunk(c)] = jnp.dot(x_s[block(i), :], w1_ref[:, chunk(c)], preferred_element_type=F32)

    def activate(i, c):
        if i < nblk:
            p = p_s[block(i), chunk(c)]
            t = jnp.tanh(p * (C0 + (C0 * C1) * (p * p)))
            a_s[block(i), chunk(c)] = (p * (0.5 + 0.5 * t)).astype(BF16)

    def residual(i):
        if 0 <= i < nblk:
            tok = block(i)
            z = x_s[tok, :].astype(F32) + jnp.dot(a_s[tok, :], w2_s[...], preferred_element_type=F32)
            z_s[tok, :] = z.astype(BF16)

    def errors(i):
        if not 0 <= i < nblk:
            return
        tok = block(i)
        logits = lax.dot_general(hc_s[...], z_s[tok, :], NT, preferred_element_type=F32)
        for t in range(2):
            lg = logits[t * SLOT:(t + 1) * SLOT]
            cls = lax.broadcasted_iota(jnp.int32, (SLOT, tb), 0)
            lg = jnp.where(cls < classes, lg, -jnp.inf)
            ex = jnp.exp(lg - lg.max(axis=0, keepdims=True))
            prob = ex * (1.0 / ex.sum(axis=0, keepdims=True))
            hot = (cls == lab_ref[t:t + 1, tok]).astype(F32)
            e = mask_ref[t:t + 1, tok].astype(F32) * (prob - hot)
            e_s[t * SLOT:(t + 1) * SLOT, tok] = e.astype(BF16)

    def back_t(i):
        if 0 <= i < nblk:
            tok = block(i)
            dzt_s[:, tok] = jnp.dot(hbt_s[...], e_s[:, tok], preferred_element_type=F32).astype(BF16)

    enter(0)
    for c in range(nchunk):
        project(0, c)
    enter(1)
    for i in range(nblk + 2):
        enter(i + 2)
        residual(i - 1)
        for c in range(nchunk):
            activate(i, c)
            project(i + 1, c)
        errors(i - 1)
        back_t(i - 2)
        if i == nblk // 2 + 1:
            pl.semaphore_wait(barrier, n - 1)
            for c in cnt_copies:
                c.start()

    def w2_part(c, carry):
        acc_s[:, chunk(c)] = jnp.dot(dzt_s[...], a_s[:, chunk(c)], preferred_element_type=F32)
        return carry

    lax.fori_loop(0, nchunk, w2_part, 0)

    for c in cnt_copies:
        c.wait()
    cnt_recv[me] = cnt_send[...]
    tot = cnt_recv[0]
    for j in range(1, n):
        tot += cnt_recv[j]
    inv = 1.0 / jnp.maximum(tot.sum(axis=1, keepdims=True), 1.0)
    inv0, inv1 = inv[0:1], inv[1:2]

    for c in range(nchunk):
        f = slice(c * fc, (c + 1) * fc)
        d = acc_s[:, f]
        tail = 2 * LANES + (model - LANES)
        d = jnp.concatenate([d[:LANES] * inv0, d[LANES:2 * LANES] * inv1,
                             d[2 * LANES:tail] * inv0, d[tail:] * inv1], axis=0)
        send2[f, :] = d.T.astype(BF16)

    def rows_of(peer):
        return send2.at[pl.ds(pl.multiple_of(peer * rows_out, rows_out), rows_out)]

    out_copies = copies(1, rows_of, recv2.at[me])
    for c in out_copies:
        c.start()

    def copies_in(c):
        return copies(2 + c, lambda peer: send1.at[c, peer], recv1.at[c, me])

    def back(i, carry):
        tok = pl.ds(pl.multiple_of(i * 2 * tb, 2 * tb), 2 * tb)
        for t in range(2):
            row = slice(t * SLOT, (t + 1) * SLOT)
            dz_s[t, tok, :] = lax.dot_general(
                e_s[row, tok], hc_s[row, :], TN, preferred_element_type=F32).astype(BF16)
        return carry

    lax.fori_loop(0, nblk // 2, back, 0)

    def w1_part(c, carry):
        for i in range(nblk):
            for t in range(2):
                da = jnp.dot(dz_s[t, block(i), :], w2t_ref[:, chunk(c)], preferred_element_type=F32)
                for r in range(0, tb, rp):
                    rows = slice(i * tb + r, i * tb + r + rp)
                    if t == 0:
                        p = p_s[rows, chunk(c)]
                        p2 = p * p
                        h = 0.5 + 0.5 * jnp.tanh(p * (C0 + (C0 * C1) * p2))
                        sl = h + (p * h * (1.0 - h)) * (2 * C0 + (6 * C0 * C1) * p2)
                        sl_s[r:r + rp, :] = sl
                    else:
                        sl = sl_s[r:r + rp, :]
                    q_s[t, rows, :] = (da[r:r + rp] * sl).astype(BF16)
        d0 = jnp.dot(xt_ref[...], q_s[0], preferred_element_type=F32) * inv0
        d1 = jnp.dot(xt_ref[...], q_s[1], preferred_element_type=F32) * inv1
        for j in range(n):
            r = slice(j * rows_in, (j + 1) * rows_in)
            send1[c, j] = jnp.concatenate([d0[r], d1[r]], axis=0).astype(BF16)
        for cp in copies_in(c):
            cp.start()
        return carry

    lax.fori_loop(0, nchunk, w1_part, 0)

    for cp in out_copies:
        cp.wait()
    recv2[me] = send2[pl.ds(pl.multiple_of(me * rows_out, rows_out), rows_out), :]
    g2 = recv2[0].astype(F32)
    for j in range(1, n):
        g2 += recv2[j].astype(F32)
    t0, t1, r = g2[:, :LANES], g2[:, LANES:2 * LANES], g2[:, 2 * LANES:]
    r_sw = pltpu.roll(r, LANES // 2, 1)
    low = lax.broadcasted_iota(jnp.int32, (1, LANES), 1) < LANES // 2

    def fold(v):
        s = v[0:8]
        for b in range(1, v.shape[0] // 8):
            s += v[8 * b:8 * b + 8]
        return s

    zero = jnp.zeros((8, LANES), F32)
    rr = fold(r * r)
    m00 = fold(t0 * t0) + jnp.where(low, rr, zero)
    m11 = fold(t1 * t1) + jnp.where(low, zero, rr)
    m01 = fold(t0 * t1) + jnp.where(low, fold(r * r_sw), zero)

    pairs = rows_out // 2
    for t, flat in ((0, flat0), (1, flat1)):
        ta_s[...] = t0 if t == 0 else t1
        tr_s[...] = r if t == 0 else r_sw
        a_e, a_o = ta_s[pl.ds(0, pairs, stride=2), :], ta_s[pl.ds(1, pairs, stride=2), :]
        r_e, r_o = tr_s[pl.ds(0, pairs, stride=2), :], tr_s[pl.ds(1, pairs, stride=2), :]
        a_w = pltpu.roll(a_o, LANES // 2, 1)
        flat[1, pl.ds(0, pairs, stride=3), :] = a_e
        flat[1, pl.ds(1, pairs, stride=3), :] = jnp.where(low, r_e, a_w)
        flat[1, pl.ds(2, pairs, stride=3), :] = jnp.where(low, a_w, pltpu.roll(r_o, LANES // 2, 1))

    wide = hidden // LANES
    for c in range(nchunk):
        for cp in copies_in(c):
            cp.wait()
        recv1[c, me] = send1[c, me]
        g1 = recv1[c, 0].astype(F32)
        for j in range(1, n):
            g1 += recv1[c, j].astype(F32)
        for b in range(fc // LANES):
            u = g1[:rows_in, b * LANES:(b + 1) * LANES]
            v = g1[rows_in:, b * LANES:(b + 1) * LANES]
            m00 += fold(u * u)
            m11 += fold(v * v)
            m01 += fold(u * v)
            flat0[0, pl.ds(c * (fc // LANES) + b, rows_in, stride=wide), :] = u
            flat1[0, pl.ds(c * (fc // LANES) + b, rows_in, stride=wide), :] = v

    row = lax.broadcasted_iota(jnp.int32, (8, LANES), 0)
    m_send[...] = jnp.where(row == 0, m00.sum(axis=0, keepdims=True),
                            jnp.where(row == 1, m01.sum(axis=0, keepdims=True),
                                      jnp.where(row == 2, m11.sum(axis=0, keepdims=True), zero)))
    m_copies = copies(2 + nchunk, lambda peer: m_send, m_recv.at[me])
    for cp in m_copies:
        cp.start()
    for cp in m_copies:
        cp.wait()
    m_recv[me] = m_send[...]
    gram = m_recv[0]
    for j in range(1, n):
        gram += m_recv[j]
    gram_ref[...] = gram


def finish(u0_ref, u1_ref, gram_ref, alpha_ref, gin_ref, gout_ref):
    gram = jnp.broadcast_to(gram_ref[...].sum(axis=1, keepdims=True), (8, LANES))
    g00, g01, g11 = gram[0:1], gram[1:2], gram[2:3]
    scale = 1.0 / ((g00 + g11) * 0.5)
    b0, b1 = (g00 - g01) * scale, (g01 - g11) * scale
    gap = jnp.zeros((1, LANES), F32)
    a0 = jnp.full((1, LANES), 0.5, F32)
    a1 = a0
    for _ in range(SOLVER_STEPS):
        gap = gap + (b0 * a0 + b1 * a1)
        ratio = jnp.exp(gap)
        a0 = 1.0 / (1.0 + ratio)
        a1 = ratio * a0
    alpha_ref[0] = a0[0, 0]
    alpha_ref[1] = a1[0, 0]
    gin_ref[...] = a0 * u0_ref[0] + a1 * u1_ref[0]
    gout_ref[...] = a0 * u0_ref[1] + a1 * u1_ref[1]


def solution(mesh):
    n = mesh.shape["data"]
    tb, rp, fc = 512, 64, 256

    def local_step(x_loc, w_in, w_out, task_heads, lab_loc, mask_loc):
        tokens, model = x_loc.shape
        hidden = w_in.shape[1]
        nchunk = hidden // fc
        piece = model * hidden // n // LANES
        rows_in, rows_out = model // n, hidden // n
        vmem = pl.BlockSpec(memory_space=pltpu.VMEM)
        u0, u1, gram = pl.pallas_call(
            functools.partial(kernel, n, tb, rp, fc),
            out_shape=(jax.ShapeDtypeStruct((2, piece, LANES), F32),
                       jax.ShapeDtypeStruct((2, piece, LANES), F32),
                       jax.ShapeDtypeStruct((8, LANES), F32)),
            in_specs=[vmem] * 6,
            out_specs=(vmem, vmem, vmem),
            scratch_shapes=[
                pltpu.VMEM((tokens, model), BF16),
                pltpu.VMEM((tb, fc), F32),
                pltpu.VMEM((tokens, hidden), BF16),
                pltpu.VMEM((tokens, hidden), F32),
                pltpu.VMEM((2 * SLOT, tokens), BF16),
                pltpu.VMEM((2, tokens, model), BF16),
                pltpu.VMEM((2 * model, tokens), BF16),
                pltpu.VMEM((tokens, model), BF16),
                pltpu.VMEM((2 * model, hidden), F32),
                pltpu.VMEM((2, tokens, fc), BF16),
                pltpu.VMEM((hidden, model), BF16),
                pltpu.VMEM((2 * SLOT, model), BF16),
                pltpu.VMEM((2 * model, 2 * SLOT), BF16),
                pltpu.VMEM((hidden, 2 * model), BF16),
                pltpu.VMEM((n, rows_out, 2 * model), BF16),
                pltpu.VMEM((nchunk, n, 2 * rows_in, fc), BF16),
                pltpu.VMEM((nchunk, n, 2 * rows_in, fc), BF16),
                pltpu.VMEM((8, LANES), F32),
                pltpu.VMEM((n, 8, LANES), F32),
                pltpu.VMEM((8, LANES), F32),
                pltpu.VMEM((n, 8, LANES), F32),
                pltpu.VMEM((rows_out, LANES), F32),
                pltpu.VMEM((rows_out, LANES), F32),
                pltpu.SemaphoreType.DMA((3 + nchunk, n)),
                pltpu.SemaphoreType.DMA((3 + nchunk, n)),
            ],
            compiler_params=pltpu.CompilerParams(
                collective_id=0, has_side_effects=True, vmem_limit_bytes=65000 * 1024),
        )(x_loc.T, w_in, w_out.T, jnp.transpose(task_heads, (2, 0, 1)), lab_loc, mask_loc)
        alpha, g_in, g_out = pl.pallas_call(
            finish,
            out_shape=(jax.ShapeDtypeStruct((2,), F32),
                       jax.ShapeDtypeStruct((piece, LANES), F32),
                       jax.ShapeDtypeStruct((piece, LANES), F32)),
            in_specs=[vmem] * 3,
            out_specs=(pl.BlockSpec(memory_space=pltpu.SMEM), vmem, vmem),
        )(u0, u1, gram)
        return alpha, g_in.reshape(-1), g_out.reshape(-1)

    return jax.shard_map(local_step, mesh=mesh, in_specs=(P("data", None), P(), P(), P(), P(None, "data"), P(None, "data")), out_specs=(P(), P("data"), P("data")), check_vma=False)
```

```python
import functools

import jax
import jax.numpy as jnp
from jax import lax
from jax.experimental import pallas as pl
from jax.experimental.pallas import tpu as pltpu
from jax.sharding import PartitionSpec as P

SOLVER_STEPS = 20
MESH = pl.DeviceIdType.MESH
F32 = jnp.float32
BF16 = jnp.bfloat16
LANES = 128
SLOT = 16
C0 = 0.7978845608028654
C1 = 0.044715

NT = (((1,), (1,)), ((), ()))
TN = (((0,), (0,)), ((), ()))


def peer_of(me, k):
    y, x, c = me // 4, (me // 2) % 2, me % 2
    return ((y + k // 4) % 2) * 4 + ((x + (k // 2) % 2) % 2) * 2 + (c + k % 2) % 2


def kernel(n, tb, rp, fc, xt_ref, w1_ref, w2t_ref, h_ref, lab_ref, mask_ref,
           flat0, flat1, gram_ref,
           x_s, sl_s, a_s, p_s, e_s, dz_s, dzt_s, z_s, acc_s, inv_s, w1h_s, w2h_s, q_s, w2_s, hc_s, hbt_s,
           send2, recv2, send1, recv1, cnt_send, cnt_recv, m_send, m_recv,
           ta_s, tr_s,
           send_sem, recv_sem):
    me = lax.axis_index("data")
    model, tokens = xt_ref.shape
    hidden = w1_ref.shape[1]
    classes = h_ref.shape[0]
    nblk, nchunk = tokens // tb, hidden // fc
    rows_in, rows_out = model // n, hidden // n

    barrier = pltpu.get_barrier_semaphore()
    for k in range(1, n):
        pl.semaphore_signal(barrier, inc=1, device_id=(peer_of(me, k),), device_id_type=MESH)

    cnt = jnp.zeros((2, LANES), F32)
    for b in range(tokens // LANES):
        cnt += mask_ref[:, b * LANES:(b + 1) * LANES].astype(F32)
    cnt_send[0:2, :] = cnt
    cnt_send[2:8, :] = jnp.zeros((6, LANES), F32)

    w2_s[...] = w2t_ref[...].T
    w1h_s[...] = (w1_ref[...].astype(F32) * 0.5).astype(BF16)
    w2h_s[...] = (w2t_ref[...].astype(F32) * 0.5).astype(BF16)
    heads = h_ref[...].astype(F32)
    gap = jnp.zeros((SLOT - classes, model), F32)
    hc = jnp.concatenate([heads[:, 0], gap, heads[:, 1], gap], axis=0)
    hc_s[...] = hc.astype(BF16)
    full = jnp.concatenate([hc, jnp.zeros((LANES - 2 * SLOT, model), F32)], axis=0).T
    lane = lax.broadcasted_iota(jnp.int32, (1, LANES), 1)
    h0 = jnp.where(lane < SLOT, full, 0.0)
    h1 = jnp.where(lane < SLOT, 0.0, full)
    hbt = jnp.concatenate([h0[:LANES], h1[:LANES], h0[LANES:], h1[LANES:]], axis=0)
    hbt_s[...] = hbt[:, :2 * SLOT].astype(BF16)

    def copies(slot, src_of, dst):
        out = []
        for k in range(1, n):
            peer = peer_of(me, k)
            out.append(pltpu.make_async_remote_copy(
                src_ref=src_of(peer), dst_ref=dst, send_sem=send_sem.at[slot, k],
                recv_sem=recv_sem.at[slot, k], device_id=(peer,), device_id_type=MESH))
        return out

    cnt_copies = copies(0, lambda peer: cnt_send, cnt_recv.at[me])

    def block(i):
        return slice(i * tb, (i + 1) * tb)

    def chunk(c):
        return pl.ds(pl.multiple_of(c * fc, fc), fc) if not isinstance(c, int) else slice(c * fc, (c + 1) * fc)

    def enter(i):
        if i < nblk:
            x_s[block(i), :] = xt_ref[:, block(i)].T

    def project(i, c):
        if i < nblk:
            p_s[block(i), chunk(c)] = jnp.dot(x_s[block(i), :], w1h_s[:, chunk(c)], preferred_element_type=F32)

    def activate(i, c):
        if i < nblk:
            p = p_s[block(i), chunk(c)]
            t = jnp.tanh(p * (2 * C0 + (8 * C0 * C1) * (p * p)))
            a_s[block(i), chunk(c)] = (p * (1.0 + t)).astype(BF16)

    def residual(i):
        if 0 <= i < nblk:
            tok = block(i)
            z = x_s[tok, :].astype(F32) + jnp.dot(a_s[tok, :], w2_s[...], preferred_element_type=F32)
            z_s[tok, :] = z.astype(BF16)

    def errors(i):
        if not 0 <= i < nblk:
            return
        tok = block(i)
        logits = lax.dot_general(hc_s[...], z_s[tok, :], NT, preferred_element_type=F32)
        for t in range(2):
            lg = logits[t * SLOT:(t + 1) * SLOT]
            cls = lax.broadcasted_iota(jnp.int32, (SLOT, tb), 0)
            lg = jnp.where(cls < classes, lg, -jnp.inf)
            ex = jnp.exp(lg - lg.max(axis=0, keepdims=True))
            prob = ex * (1.0 / ex.sum(axis=0, keepdims=True))
            hot = (cls == lab_ref[t:t + 1, tok]).astype(F32)
            e = mask_ref[t:t + 1, tok].astype(F32) * (prob - hot)
            e_s[t * SLOT:(t + 1) * SLOT, tok] = e.astype(BF16)

    def back_t(i):
        if 0 <= i < nblk:
            tok = block(i)
            dzt_s[:, tok] = jnp.dot(hbt_s[...], e_s[:, tok], preferred_element_type=F32).astype(BF16)

    def back(i):
        if 0 <= i < nblk:
            tok = block(i)
            for t in range(2):
                row = slice(t * SLOT, (t + 1) * SLOT)
                dz_s[t, tok, :] = lax.dot_general(
                    e_s[row, tok], hc_s[row, :], TN, preferred_element_type=F32).astype(BF16)

    enter(0)
    for c in range(nchunk):
        project(0, c)
    enter(1)
    for i in range(nblk + 2):
        enter(i + 2)
        residual(i - 1)
        for c in range(nchunk):
            activate(i, c)
            project(i + 1, c)
        errors(i - 1)
        back_t(i - 2)
        back(i - 2)
        if i == min(3, nblk):
            pl.semaphore_wait(barrier, n - 1)
            for c in cnt_copies:
                c.start()

    @pl.when(me != n)
    def _():
        for c in cnt_copies:
            c.wait()
        cnt_recv[me] = cnt_send[...]
        tot = cnt_recv[0]
        for j in range(1, n):
            tot += cnt_recv[j]
        inv = 1.0 / jnp.maximum(tot.sum(axis=1, keepdims=True), 1.0)
        inv_s[...] = jnp.broadcast_to(inv, (8, LANES))

    my_y, my_x, my_c = me // 4, (me // 2) % 2, me % 2

    def order(s):
        return my_y * s + (1 - my_y) * (nchunk - 1 - s)

    def w2_products(s):
        acc_s[s % 2] = jnp.dot(dzt_s[...], a_s[:, chunk(order(s))], preferred_element_type=F32)

    def w2_scale(s):
        inv0, inv1 = inv_s[0:1, 0:1], inv_s[1:2, 0:1]
        d = acc_s[s % 2]
        tail = 2 * LANES + (model - LANES)
        d = jnp.concatenate([d[:LANES] * inv0, d[LANES:2 * LANES] * inv1,
                             d[2 * LANES:tail] * inv0, d[tail:] * inv1], axis=0)
        send2[chunk(order(s)), :] = d.T.astype(BF16)

    def rows_of(peer):
        return send2.at[pl.ds(pl.multiple_of(peer * rows_out, rows_out), rows_out)]

    out_copies = copies(1, rows_of, recv2.at[me])

    def w2_send(s):
        if s == nchunk - 1:
            for k in (2, 3, 1):
                out_copies[k - 1].start()
            return
        to_x = (1 - my_y) * (1 - s) + my_y * s
        for to_c in range(2):
            peer = (1 - my_y) * 4 + to_x * 2 + to_c
            k = 4 + 2 * ((my_x + to_x) % 2) + (my_c + to_c) % 2
            pltpu.make_async_remote_copy(
                src_ref=rows_of(peer), dst_ref=recv2.at[me], send_sem=send_sem.at[1, k],
                recv_sem=recv_sem.at[1, k], device_id=(peer,), device_id_type=MESH).start()

    for s in range(nchunk + 1):
        @pl.when(me != n + 1 + s)
        def _():
            if s > 0:
                w2_scale(s - 1)
                w2_send(s - 1)
            if s < nchunk:
                w2_products(s)

    inv0, inv1 = inv_s[0:1, 0:1], inv_s[1:2, 0:1]

    def copies_in(c):
        return copies(2 + c, lambda peer: send1.at[c, peer], recv1.at[c, me])

    def w1_part(c, carry):
        for i in range(nblk):
            for t in range(2):
                da = jnp.dot(dz_s[t, block(i), :], w2h_s[:, chunk(c)], preferred_element_type=F32)
                for r in range(0, tb, rp):
                    rows = slice(i * tb + r, i * tb + r + rp)
                    if t == 0:
                        p = p_s[rows, chunk(c)]
                        p2 = p * p
                        th = jnp.tanh(p * (2 * C0 + (8 * C0 * C1) * p2))
                        sl = (1.0 + th) * (1.0 + p * ((1.0 - th) * (2 * C0 + (24 * C0 * C1) * p2)))
                        sl_s[r:r + rp, :] = sl
                    else:
                        sl = sl_s[r:r + rp, :]
                    q_s[t, rows, :] = (da[r:r + rp] * sl).astype(BF16)
        d0 = jnp.dot(xt_ref[...], q_s[0], preferred_element_type=F32) * inv0
        d1 = jnp.dot(xt_ref[...], q_s[1], preferred_element_type=F32) * inv1
        for j in range(n):
            r = slice(j * rows_in, (j + 1) * rows_in)
            send1[c, j] = jnp.concatenate([d0[r], d1[r]], axis=0).astype(BF16)
        now = copies_in(c)
        for k in (6, 7, 4, 5, 2, 3, 1):
            now[k - 1].start()
        return carry

    lax.fori_loop(0, nchunk, w1_part, 0)

    for cp in out_copies:
        cp.wait()
    recv2[me] = send2[pl.ds(pl.multiple_of(me * rows_out, rows_out), rows_out), :]
    g2 = recv2[0].astype(F32)
    for j in range(1, n):
        g2 += recv2[j].astype(F32)
    t0, t1, r = g2[:, :LANES], g2[:, LANES:2 * LANES], g2[:, 2 * LANES:]
    r_sw = pltpu.roll(r, LANES // 2, 1)
    low = lax.broadcasted_iota(jnp.int32, (1, LANES), 1) < LANES // 2

    def fold(v):
        s = v[0:8]
        for b in range(1, v.shape[0] // 8):
            s += v[8 * b:8 * b + 8]
        return s

    zero = jnp.zeros((8, LANES), F32)
    rr = fold(r * r)
    m00 = fold(t0 * t0) + jnp.where(low, rr, zero)
    m11 = fold(t1 * t1) + jnp.where(low, zero, rr)
    m01 = fold(t0 * t1) + jnp.where(low, fold(r * r_sw), zero)

    pairs = rows_out // 2
    for t, flat in ((0, flat0), (1, flat1)):
        ta_s[...] = t0 if t == 0 else t1
        tr_s[...] = r if t == 0 else r_sw
        a_e, a_o = ta_s[pl.ds(0, pairs, stride=2), :], ta_s[pl.ds(1, pairs, stride=2), :]
        r_e, r_o = tr_s[pl.ds(0, pairs, stride=2), :], tr_s[pl.ds(1, pairs, stride=2), :]
        a_w = pltpu.roll(a_o, LANES // 2, 1)
        flat[1, pl.ds(0, pairs, stride=3), :] = a_e
        flat[1, pl.ds(1, pairs, stride=3), :] = jnp.where(low, r_e, a_w)
        flat[1, pl.ds(2, pairs, stride=3), :] = jnp.where(low, a_w, pltpu.roll(r_o, LANES // 2, 1))

    wide = hidden // LANES
    for c in range(nchunk):
        for cp in copies_in(c):
            cp.wait()
        recv1[c, me] = send1[c, me]
        g1 = recv1[c, 0].astype(F32)
        for j in range(1, n):
            g1 += recv1[c, j].astype(F32)
        for b in range(fc // LANES):
            u = g1[:rows_in, b * LANES:(b + 1) * LANES]
            v = g1[rows_in:, b * LANES:(b + 1) * LANES]
            m00 += fold(u * u)
            m11 += fold(v * v)
            m01 += fold(u * v)
            flat0[0, pl.ds(c * (fc // LANES) + b, rows_in, stride=wide), :] = u
            flat1[0, pl.ds(c * (fc // LANES) + b, rows_in, stride=wide), :] = v

    row = lax.broadcasted_iota(jnp.int32, (8, LANES), 0)
    m_send[...] = jnp.where(row == 0, m00.sum(axis=0, keepdims=True),
                            jnp.where(row == 1, m01.sum(axis=0, keepdims=True),
                                      jnp.where(row == 2, m11.sum(axis=0, keepdims=True), zero)))
    m_copies = copies(2 + nchunk, lambda peer: m_send, m_recv.at[me])
    for cp in m_copies:
        cp.start()
    for cp in m_copies:
        cp.wait()
    m_recv[me] = m_send[...]
    gram = m_recv[0]
    for j in range(1, n):
        gram += m_recv[j]
    gram_ref[...] = gram


def finish(u0_ref, u1_ref, gram_ref, alpha_ref, gin_ref, gout_ref):
    gram = jnp.broadcast_to(gram_ref[...].sum(axis=1, keepdims=True), (8, LANES))
    g00, g01, g11 = gram[0:1], gram[1:2], gram[2:3]
    scale = 1.0 / ((g00 + g11) * 0.5)
    b0, b1 = (g00 - g01) * scale, (g01 - g11) * scale
    shift, turn = 0.25 * (b0 + b1), 0.25 * (b1 - b0)
    h = jnp.zeros((1, LANES), F32)
    for _ in range(SOLVER_STEPS):
        h = (h + shift) + turn * jnp.tanh(h)
    ratio = jnp.exp(h + h)
    a0 = 1.0 / (1.0 + ratio)
    a1 = ratio * a0
    alpha_ref[0] = a0[0, 0]
    alpha_ref[1] = a1[0, 0]
    gin_ref[...] = a0 * u0_ref[0] + a1 * u1_ref[0]
    gout_ref[...] = a0 * u0_ref[1] + a1 * u1_ref[1]


def solution(mesh):
    n = mesh.shape["data"]
    tb, rp, fc = 512, 64, 256

    def local_step(x_loc, w_in, w_out, task_heads, lab_loc, mask_loc):
        tokens, model = x_loc.shape
        hidden = w_in.shape[1]
        nchunk = hidden // fc
        piece = model * hidden // n // LANES
        rows_in, rows_out = model // n, hidden // n
        vmem = pl.BlockSpec(memory_space=pltpu.VMEM)
        u0, u1, gram = pl.pallas_call(
            functools.partial(kernel, n, tb, rp, fc),
            out_shape=(jax.ShapeDtypeStruct((2, piece, LANES), F32),
                       jax.ShapeDtypeStruct((2, piece, LANES), F32),
                       jax.ShapeDtypeStruct((8, LANES), F32)),
            in_specs=[vmem] * 6,
            out_specs=(vmem, vmem, vmem),
            scratch_shapes=[
                pltpu.VMEM((tokens, model), BF16),
                pltpu.VMEM((tb, fc), F32),
                pltpu.VMEM((tokens, hidden), BF16),
                pltpu.VMEM((tokens, hidden), F32),
                pltpu.VMEM((2 * SLOT, tokens), BF16),
                pltpu.VMEM((2, tokens, model), BF16),
                pltpu.VMEM((2 * model, tokens), BF16),
                pltpu.VMEM((tokens, model), BF16),
                pltpu.VMEM((2, 2 * model, fc), F32),
                pltpu.VMEM((8, LANES), F32),
                pltpu.VMEM((model, hidden), BF16),
                pltpu.VMEM((model, hidden), BF16),
                pltpu.VMEM((2, tokens, fc), BF16),
                pltpu.VMEM((hidden, model), BF16),
                pltpu.VMEM((2 * SLOT, model), BF16),
                pltpu.VMEM((2 * model, 2 * SLOT), BF16),
                pltpu.VMEM((hidden, 2 * model), BF16),
                pltpu.VMEM((n, rows_out, 2 * model), BF16),
                pltpu.VMEM((nchunk, n, 2 * rows_in, fc), BF16),
                pltpu.VMEM((nchunk, n, 2 * rows_in, fc), BF16),
                pltpu.VMEM((8, LANES), F32),
                pltpu.VMEM((n, 8, LANES), F32),
                pltpu.VMEM((8, LANES), F32),
                pltpu.VMEM((n, 8, LANES), F32),
                pltpu.VMEM((rows_out, LANES), F32),
                pltpu.VMEM((rows_out, LANES), F32),
                pltpu.SemaphoreType.DMA((3 + nchunk, n)),
                pltpu.SemaphoreType.DMA((3 + nchunk, n)),
            ],
            compiler_params=pltpu.CompilerParams(
                collective_id=0, has_side_effects=True, vmem_limit_bytes=65000 * 1024),
        )(x_loc.T, w_in, w_out.T, jnp.transpose(task_heads, (2, 0, 1)), lab_loc, mask_loc)
        alpha, g_in, g_out = pl.pallas_call(
            finish,
            out_shape=(jax.ShapeDtypeStruct((2,), F32),
                       jax.ShapeDtypeStruct((piece, LANES), F32),
                       jax.ShapeDtypeStruct((piece, LANES), F32)),
            in_specs=[vmem] * 3,
            out_specs=(pl.BlockSpec(memory_space=pltpu.SMEM), vmem, vmem),
        )(u0, u1, gram)
        return alpha, g_in.reshape(-1), g_out.reshape(-1)

    return jax.shard_map(local_step, mesh=mesh, in_specs=(P("data", None), P(), P(), P(), P(None, "data"), P(None, "data")), out_specs=(P(), P("data"), P("data")), check_vma=False)
```

```python
import functools

import jax
import jax.numpy as jnp
from jax import lax
from jax.experimental import pallas as pl
from jax.experimental.pallas import tpu as pltpu
from jax.sharding import PartitionSpec as P

SOLVER_STEPS = 20
MESH = pl.DeviceIdType.MESH
F32 = jnp.float32
BF16 = jnp.bfloat16
LANES = 128
SLOT = 16
C0 = 0.7978845608028654
C1 = 0.044715

NT = (((1,), (1,)), ((), ()))
TN = (((0,), (0,)), ((), ()))


def peer_of(me, k):
    y, x, c = me // 4, (me // 2) % 2, me % 2
    return ((y + k // 4) % 2) * 4 + ((x + (k // 2) % 2) % 2) * 2 + (c + k % 2) % 2


def kernel(n, tb, rp, fc, xt_ref, w1_ref, w2t_ref, h_ref, lab_ref, mask_ref,
           flat0, flat1, gram_ref,
           x_s, sl_s, a_s, p_s, e_s, dz_s, dzt_s, z_s, acc_s, inv_s, w1h_s, w2h_s, q_s, w2_s, hc_s, hbt_s,
           send2, recv2, send1, recv1, cnt_send, cnt_recv, m_send, m_recv,
           ta_s, tr_s,
           send_sem, recv_sem):
    me = lax.axis_index("data")
    model, tokens = xt_ref.shape
    hidden = w1_ref.shape[1]
    classes = h_ref.shape[0]
    nblk, nchunk = tokens // tb, hidden // fc
    rows_in, rows_out = model // n, hidden // n

    barrier = pltpu.get_barrier_semaphore()
    for k in range(1, n):
        pl.semaphore_signal(barrier, inc=1, device_id=(peer_of(me, k),), device_id_type=MESH)

    cnt = jnp.zeros((2, LANES), F32)
    for b in range(tokens // LANES):
        cnt += mask_ref[:, b * LANES:(b + 1) * LANES].astype(F32)
    cnt_send[0:2, :] = cnt
    cnt_send[2:8, :] = jnp.zeros((6, LANES), F32)

    w2_s[...] = w2t_ref[...].T
    w1h_s[...] = (w1_ref[...].astype(F32) * 0.5).astype(BF16)
    w2h_s[...] = (w2t_ref[...].astype(F32) * 0.5).astype(BF16)
    heads = h_ref[...].astype(F32)
    gap = jnp.zeros((SLOT - classes, model), F32)
    hc = jnp.concatenate([heads[:, 0], gap, heads[:, 1], gap], axis=0)
    hc_s[...] = hc.astype(BF16)
    full = jnp.concatenate([hc, jnp.zeros((LANES - 2 * SLOT, model), F32)], axis=0).T
    lane = lax.broadcasted_iota(jnp.int32, (1, LANES), 1)
    h0 = jnp.where(lane < SLOT, full, 0.0)
    h1 = jnp.where(lane < SLOT, 0.0, full)
    hbt = jnp.concatenate([h0[:LANES], h1[:LANES], h0[LANES:], h1[LANES:]], axis=0)
    hbt_s[...] = hbt[:, :2 * SLOT].astype(BF16)

    def copies(slot, src_of, dst):
        out = []
        for k in range(1, n):
            peer = peer_of(me, k)
            out.append(pltpu.make_async_remote_copy(
                src_ref=src_of(peer), dst_ref=dst, send_sem=send_sem.at[slot, k],
                recv_sem=recv_sem.at[slot, k], device_id=(peer,), device_id_type=MESH))
        return out

    cnt_copies = copies(0, lambda peer: cnt_send, cnt_recv.at[me])

    def block(i):
        return slice(i * tb, (i + 1) * tb)

    def chunk(c):
        return pl.ds(pl.multiple_of(c * fc, fc), fc) if not isinstance(c, int) else slice(c * fc, (c + 1) * fc)

    def enter(i):
        if i < nblk:
            x_s[block(i), :] = xt_ref[:, block(i)].T

    def project(i, c):
        if i < nblk:
            p_s[block(i), chunk(c)] = jnp.dot(x_s[block(i), :], w1h_s[:, chunk(c)], preferred_element_type=F32)

    def activate(i, c):
        if i < nblk:
            p = p_s[block(i), chunk(c)]
            t = jnp.tanh(p * (2 * C0 + (8 * C0 * C1) * (p * p)))
            a_s[block(i), chunk(c)] = (p * (1.0 + t)).astype(BF16)

    def residual(i):
        if 0 <= i < nblk:
            tok = block(i)
            z = x_s[tok, :].astype(F32) + jnp.dot(a_s[tok, :], w2_s[...], preferred_element_type=F32)
            z_s[tok, :] = z.astype(BF16)

    def errors(i):
        if not 0 <= i < nblk:
            return
        tok = block(i)
        logits = lax.dot_general(hc_s[...], z_s[tok, :], NT, preferred_element_type=F32)
        for t in range(2):
            lg = logits[t * SLOT:(t + 1) * SLOT]
            cls = lax.broadcasted_iota(jnp.int32, (SLOT, tb), 0)
            lg = jnp.where(cls < classes, lg, -jnp.inf)
            ex = jnp.exp(lg - lg.max(axis=0, keepdims=True))
            prob = ex * (1.0 / ex.sum(axis=0, keepdims=True))
            hot = (cls == lab_ref[t:t + 1, tok]).astype(F32)
            e = mask_ref[t:t + 1, tok].astype(F32) * (prob - hot)
            e_s[t * SLOT:(t + 1) * SLOT, tok] = e.astype(BF16)

    def back_t(i):
        if 0 <= i < nblk:
            tok = block(i)
            dzt_s[:, tok] = jnp.dot(hbt_s[...], e_s[:, tok], preferred_element_type=F32).astype(BF16)

    def back(i):
        if 0 <= i < nblk:
            tok = block(i)
            for t in range(2):
                row = slice(t * SLOT, (t + 1) * SLOT)
                dz_s[t, tok, :] = lax.dot_general(
                    e_s[row, tok], hc_s[row, :], TN, preferred_element_type=F32).astype(BF16)

    enter(0)
    for c in range(nchunk):
        project(0, c)
    enter(1)
    for i in range(nblk + 2):
        enter(i + 2)
        residual(i - 1)
        for c in range(nchunk):
            activate(i, c)
            project(i + 1, c)
        errors(i - 1)
        back_t(i - 2)
        if i < nblk:
            back(i - 2)
        if i == min(3, nblk):
            pl.semaphore_wait(barrier, n - 1)
            for c in cnt_copies:
                c.start()

    @pl.when(me != n)
    def _():
        for c in cnt_copies:
            c.wait()
        cnt_recv[me] = cnt_send[...]
        tot = cnt_recv[0]
        for j in range(1, n):
            tot += cnt_recv[j]
        inv = 1.0 / jnp.maximum(tot.sum(axis=1, keepdims=True), 1.0)
        inv_s[...] = jnp.broadcast_to(inv, (8, LANES))

    my_y, my_x, my_c = me // 4, (me // 2) % 2, me % 2

    def order(s):
        return my_y * s + (1 - my_y) * (nchunk - 1 - s)

    def w2_products(s):
        acc_s[s % 2] = jnp.dot(dzt_s[...], a_s[:, chunk(order(s))], preferred_element_type=F32)

    def w2_scale(s):
        inv0, inv1 = inv_s[0:1, 0:1], inv_s[1:2, 0:1]
        d = acc_s[s % 2]
        tail = 2 * LANES + (model - LANES)
        d = jnp.concatenate([d[:LANES] * inv0, d[LANES:2 * LANES] * inv1,
                             d[2 * LANES:tail] * inv0, d[tail:] * inv1], axis=0)
        send2[chunk(order(s)), :] = d.T.astype(BF16)

    def rows_of(peer):
        return send2.at[pl.ds(pl.multiple_of(peer * rows_out, rows_out), rows_out)]

    out_copies = copies(1, rows_of, recv2.at[me])

    def w2_send(s):
        if s == nchunk - 1:
            for k in (2, 3, 1):
                out_copies[k - 1].start()
            return
        to_x = (1 - my_y) * (1 - s) + my_y * s
        for to_c in range(2):
            peer = (1 - my_y) * 4 + to_x * 2 + to_c
            k = 4 + 2 * ((my_x + to_x) % 2) + (my_c + to_c) % 2
            pltpu.make_async_remote_copy(
                src_ref=rows_of(peer), dst_ref=recv2.at[me], send_sem=send_sem.at[1, k],
                recv_sem=recv_sem.at[1, k], device_id=(peer,), device_id_type=MESH).start()

    for s in range(nchunk + 1):
        @pl.when(me != n + 1 + s)
        def _():
            if s > 0:
                w2_scale(s - 1)
                w2_send(s - 1)
            if s < nchunk:
                w2_products(s)
            if s == nchunk:
                back(nblk - 2)
                back(nblk - 1)

    inv0, inv1 = inv_s[0:1, 0:1], inv_s[1:2, 0:1]

    def copies_in(c):
        return copies(2 + c, lambda peer: send1.at[c, peer], recv1.at[c, me])

    def w1_part(c, carry):
        for i in range(nblk):
            for t in range(2):
                da = jnp.dot(dz_s[t, block(i), :], w2h_s[:, chunk(c)], preferred_element_type=F32)
                for r in range(0, tb, rp):
                    rows = slice(i * tb + r, i * tb + r + rp)
                    if t == 0:
                        p = p_s[rows, chunk(c)]
                        p2 = p * p
                        th = jnp.tanh(p * (2 * C0 + (8 * C0 * C1) * p2))
                        sl = (1.0 + th) * (1.0 + p * ((1.0 - th) * (2 * C0 + (24 * C0 * C1) * p2)))
                        sl_s[r:r + rp, :] = sl
                    else:
                        sl = sl_s[r:r + rp, :]
                    q_s[t, rows, :] = (da[r:r + rp] * sl).astype(BF16)
        d0 = jnp.dot(xt_ref[...], q_s[0], preferred_element_type=F32) * inv0
        d1 = jnp.dot(xt_ref[...], q_s[1], preferred_element_type=F32) * inv1
        for j in range(n):
            r = slice(j * rows_in, (j + 1) * rows_in)
            send1[c, j] = jnp.concatenate([d0[r], d1[r]], axis=0).astype(BF16)
        now = copies_in(c)
        for k in (6, 7, 4, 5, 2, 3, 1):
            now[k - 1].start()
        return carry

    lax.fori_loop(0, nchunk, w1_part, 0)

    for cp in out_copies:
        cp.wait()
    recv2[me] = send2[pl.ds(pl.multiple_of(me * rows_out, rows_out), rows_out), :]
    g2 = recv2[0].astype(F32)
    for j in range(1, n):
        g2 += recv2[j].astype(F32)
    t0, t1, r = g2[:, :LANES], g2[:, LANES:2 * LANES], g2[:, 2 * LANES:]
    r_sw = pltpu.roll(r, LANES // 2, 1)
    low = lax.broadcasted_iota(jnp.int32, (1, LANES), 1) < LANES // 2

    def fold(v):
        s = v[0:8]
        for b in range(1, v.shape[0] // 8):
            s += v[8 * b:8 * b + 8]
        return s

    zero = jnp.zeros((8, LANES), F32)
    rr = fold(r * r)
    m00 = fold(t0 * t0) + jnp.where(low, rr, zero)
    m11 = fold(t1 * t1) + jnp.where(low, zero, rr)
    m01 = fold(t0 * t1) + jnp.where(low, fold(r * r_sw), zero)

    pairs = rows_out // 2
    for t, flat in ((0, flat0), (1, flat1)):
        ta_s[...] = t0 if t == 0 else t1
        tr_s[...] = r if t == 0 else r_sw
        a_e, a_o = ta_s[pl.ds(0, pairs, stride=2), :], ta_s[pl.ds(1, pairs, stride=2), :]
        r_e, r_o = tr_s[pl.ds(0, pairs, stride=2), :], tr_s[pl.ds(1, pairs, stride=2), :]
        a_w = pltpu.roll(a_o, LANES // 2, 1)
        flat[1, pl.ds(0, pairs, stride=3), :] = a_e
        flat[1, pl.ds(1, pairs, stride=3), :] = jnp.where(low, r_e, a_w)
        flat[1, pl.ds(2, pairs, stride=3), :] = jnp.where(low, a_w, pltpu.roll(r_o, LANES // 2, 1))

    wide = hidden // LANES
    for c in range(nchunk):
        for cp in copies_in(c):
            cp.wait()
        recv1[c, me] = send1[c, me]
        g1 = recv1[c, 0].astype(F32)
        for j in range(1, n):
            g1 += recv1[c, j].astype(F32)
        for b in range(fc // LANES):
            u = g1[:rows_in, b * LANES:(b + 1) * LANES]
            v = g1[rows_in:, b * LANES:(b + 1) * LANES]
            m00 += fold(u * u)
            m11 += fold(v * v)
            m01 += fold(u * v)
            flat0[0, pl.ds(c * (fc // LANES) + b, rows_in, stride=wide), :] = u
            flat1[0, pl.ds(c * (fc // LANES) + b, rows_in, stride=wide), :] = v

    row = lax.broadcasted_iota(jnp.int32, (8, LANES), 0)
    m_send[...] = jnp.where(row == 0, m00.sum(axis=0, keepdims=True),
                            jnp.where(row == 1, m01.sum(axis=0, keepdims=True),
                                      jnp.where(row == 2, m11.sum(axis=0, keepdims=True), zero)))
    m_copies = copies(2 + nchunk, lambda peer: m_send, m_recv.at[me])
    for cp in m_copies:
        cp.start()
    for cp in m_copies:
        cp.wait()
    m_recv[me] = m_send[...]
    gram = m_recv[0]
    for j in range(1, n):
        gram += m_recv[j]
    gram_ref[...] = gram


def finish(u0_ref, u1_ref, gram_ref, alpha_ref, gin_ref, gout_ref):
    gram = jnp.broadcast_to(gram_ref[...].sum(axis=1, keepdims=True), (8, LANES))
    g00, g01, g11 = gram[0:1], gram[1:2], gram[2:3]
    scale = 1.0 / ((g00 + g11) * 0.5)
    b0, b1 = (g00 - g01) * scale, (g01 - g11) * scale
    shift, turn = 0.25 * (b0 + b1), 0.25 * (b1 - b0)
    h = jnp.zeros((1, LANES), F32)
    for _ in range(SOLVER_STEPS):
        h = (h + shift) + turn * jnp.tanh(h)
    ratio = jnp.exp(h + h)
    a0 = 1.0 / (1.0 + ratio)
    a1 = ratio * a0
    alpha_ref[0] = a0[0, 0]
    alpha_ref[1] = a1[0, 0]
    gin_ref[...] = a0 * u0_ref[0] + a1 * u1_ref[0]
    gout_ref[...] = a0 * u0_ref[1] + a1 * u1_ref[1]


def solution(mesh):
    n = mesh.shape["data"]
    tb, rp, fc = 512, 64, 256

    def local_step(x_loc, w_in, w_out, task_heads, lab_loc, mask_loc):
        tokens, model = x_loc.shape
        hidden = w_in.shape[1]
        nchunk = hidden // fc
        piece = model * hidden // n // LANES
        rows_in, rows_out = model // n, hidden // n
        vmem = pl.BlockSpec(memory_space=pltpu.VMEM)
        u0, u1, gram = pl.pallas_call(
            functools.partial(kernel, n, tb, rp, fc),
            out_shape=(jax.ShapeDtypeStruct((2, piece, LANES), F32),
                       jax.ShapeDtypeStruct((2, piece, LANES), F32),
                       jax.ShapeDtypeStruct((8, LANES), F32)),
            in_specs=[vmem] * 6,
            out_specs=(vmem, vmem, vmem),
            scratch_shapes=[
                pltpu.VMEM((tokens, model), BF16),
                pltpu.VMEM((tb, fc), F32),
                pltpu.VMEM((tokens, hidden), BF16),
                pltpu.VMEM((tokens, hidden), F32),
                pltpu.VMEM((2 * SLOT, tokens), BF16),
                pltpu.VMEM((2, tokens, model), BF16),
                pltpu.VMEM((2 * model, tokens), BF16),
                pltpu.VMEM((tokens, model), BF16),
                pltpu.VMEM((2, 2 * model, fc), F32),
                pltpu.VMEM((8, LANES), F32),
                pltpu.VMEM((model, hidden), BF16),
                pltpu.VMEM((model, hidden), BF16),
                pltpu.VMEM((2, tokens, fc), BF16),
                pltpu.VMEM((hidden, model), BF16),
                pltpu.VMEM((2 * SLOT, model), BF16),
                pltpu.VMEM((2 * model, 2 * SLOT), BF16),
                pltpu.VMEM((hidden, 2 * model), BF16),
                pltpu.VMEM((n, rows_out, 2 * model), BF16),
                pltpu.VMEM((nchunk, n, 2 * rows_in, fc), BF16),
                pltpu.VMEM((nchunk, n, 2 * rows_in, fc), BF16),
                pltpu.VMEM((8, LANES), F32),
                pltpu.VMEM((n, 8, LANES), F32),
                pltpu.VMEM((8, LANES), F32),
                pltpu.VMEM((n, 8, LANES), F32),
                pltpu.VMEM((rows_out, LANES), F32),
                pltpu.VMEM((rows_out, LANES), F32),
                pltpu.SemaphoreType.DMA((3 + nchunk, n)),
                pltpu.SemaphoreType.DMA((3 + nchunk, n)),
            ],
            compiler_params=pltpu.CompilerParams(
                collective_id=0, has_side_effects=True, vmem_limit_bytes=65000 * 1024),
        )(x_loc.T, w_in, w_out.T, jnp.transpose(task_heads, (2, 0, 1)), lab_loc, mask_loc)
        alpha, g_in, g_out = pl.pallas_call(
            finish,
            out_shape=(jax.ShapeDtypeStruct((2,), F32),
                       jax.ShapeDtypeStruct((piece, LANES), F32),
                       jax.ShapeDtypeStruct((piece, LANES), F32)),
            in_specs=[vmem] * 3,
            out_specs=(pl.BlockSpec(memory_space=pltpu.SMEM), vmem, vmem),
        )(u0, u1, gram)
        return alpha, g_in.reshape(-1), g_out.reshape(-1)

    return jax.shard_map(local_step, mesh=mesh, in_specs=(P("data", None), P(), P(), P(), P(None, "data"), P(None, "data")), out_specs=(P(), P("data"), P("data")), check_vma=False)
```

```python
import functools

import jax
import jax.numpy as jnp
from jax import lax
from jax.experimental import pallas as pl
from jax.experimental.pallas import tpu as pltpu
from jax.sharding import PartitionSpec as P

SOLVER_STEPS = 20
MESH = pl.DeviceIdType.MESH
F32 = jnp.float32
BF16 = jnp.bfloat16
LANES = 128
SLOT = 16
C0 = 0.7978845608028654
C1 = 0.044715

NT = (((1,), (1,)), ((), ()))
TN = (((0,), (0,)), ((), ()))


def peer_of(me, k):
    y, x, c = me // 4, (me // 2) % 2, me % 2
    return ((y + k // 4) % 2) * 4 + ((x + (k // 2) % 2) % 2) * 2 + (c + k % 2) % 2


def kernel(n, tb, rp, fc, xt_ref, w1_ref, w2t_ref, h_ref, lab_ref, mask_ref,
           u0_ref, u1_ref, gram_ref,
           x_s, sl_s, a_s, p_s, e_s, dz_s, dzt_s, z_s, acc_s, inv_s, w1h_s, w2h_s, q_s, w2_s, hc_s, hbt_s,
           send2, recv2, send1, recv1, cnt_send, cnt_recv, m_send, m_recv,
           flat0, flat1, ta_s, tr_s,
           send_sem, recv_sem, save_sem):
    me = lax.axis_index("data")
    model, tokens = xt_ref.shape
    hidden = w1_ref.shape[1]
    classes = h_ref.shape[0]
    nblk, nchunk = tokens // tb, hidden // fc
    rows_in, rows_out = model // n, hidden // n

    barrier = pltpu.get_barrier_semaphore()
    for k in range(1, n):
        pl.semaphore_signal(barrier, inc=1, device_id=(peer_of(me, k),), device_id_type=MESH)

    cnt = jnp.zeros((2, LANES), F32)
    for b in range(tokens // LANES):
        cnt += mask_ref[:, b * LANES:(b + 1) * LANES].astype(F32)
    cnt_send[0:2, :] = cnt
    cnt_send[2:8, :] = jnp.zeros((6, LANES), F32)

    w2_s[...] = w2t_ref[...].T
    w1h_s[...] = (w1_ref[...].astype(F32) * 0.5).astype(BF16)
    w2h_s[...] = (w2t_ref[...].astype(F32) * 0.5).astype(BF16)
    heads = h_ref[...].astype(F32)
    gap = jnp.zeros((SLOT - classes, model), F32)
    hc = jnp.concatenate([heads[:, 0], gap, heads[:, 1], gap], axis=0)
    hc_s[...] = hc.astype(BF16)
    full = jnp.concatenate([hc, jnp.zeros((LANES - 2 * SLOT, model), F32)], axis=0).T
    lane = lax.broadcasted_iota(jnp.int32, (1, LANES), 1)
    h0 = jnp.where(lane < SLOT, full, 0.0)
    h1 = jnp.where(lane < SLOT, 0.0, full)
    hbt = jnp.concatenate([h0[:LANES], h1[:LANES], h0[LANES:], h1[LANES:]], axis=0)
    hbt_s[...] = hbt[:, :2 * SLOT].astype(BF16)

    def copies(slot, src_of, dst):
        out = []
        for k in range(1, n):
            peer = peer_of(me, k)
            out.append(pltpu.make_async_remote_copy(
                src_ref=src_of(peer), dst_ref=dst, send_sem=send_sem.at[slot, k],
                recv_sem=recv_sem.at[slot, k], device_id=(peer,), device_id_type=MESH))
        return out

    cnt_copies = copies(0, lambda peer: cnt_send, cnt_recv.at[me])

    def block(i):
        return slice(i * tb, (i + 1) * tb)

    def chunk(c):
        return pl.ds(pl.multiple_of(c * fc, fc), fc) if not isinstance(c, int) else slice(c * fc, (c + 1) * fc)

    def enter(i):
        if i < nblk:
            x_s[block(i), :] = xt_ref[:, block(i)].T

    def project(i, c):
        if i < nblk:
            p_s[block(i), chunk(c)] = jnp.dot(x_s[block(i), :], w1h_s[:, chunk(c)], preferred_element_type=F32)

    def activate(i, c):
        if i < nblk:
            p = p_s[block(i), chunk(c)]
            t = jnp.tanh(p * (2 * C0 + (8 * C0 * C1) * (p * p)))
            a_s[block(i), chunk(c)] = (p * (1.0 + t)).astype(BF16)

    def residual(i):
        if 0 <= i < nblk:
            tok = block(i)
            z = x_s[tok, :].astype(F32) + jnp.dot(a_s[tok, :], w2_s[...], preferred_element_type=F32)
            z_s[tok, :] = z.astype(BF16)

    def errors(i):
        if not 0 <= i < nblk:
            return
        tok = block(i)
        logits = lax.dot_general(hc_s[...], z_s[tok, :], NT, preferred_element_type=F32)
        for t in range(2):
            lg = logits[t * SLOT:(t + 1) * SLOT]
            cls = lax.broadcasted_iota(jnp.int32, (SLOT, tb), 0)
            lg = jnp.where(cls < classes, lg, -jnp.inf)
            ex = jnp.exp(lg - lg.max(axis=0, keepdims=True))
            prob = ex * (1.0 / ex.sum(axis=0, keepdims=True))
            hot = (cls == lab_ref[t:t + 1, tok]).astype(F32)
            e = mask_ref[t:t + 1, tok].astype(F32) * (prob - hot)
            e_s[t * SLOT:(t + 1) * SLOT, tok] = e.astype(BF16)

    def back_t(i):
        if 0 <= i < nblk:
            tok = block(i)
            dzt_s[:, tok] = jnp.dot(hbt_s[...], e_s[:, tok], preferred_element_type=F32).astype(BF16)

    def back(i):
        if 0 <= i < nblk:
            tok = block(i)
            for t in range(2):
                row = slice(t * SLOT, (t + 1) * SLOT)
                dz_s[t, tok, :] = lax.dot_general(
                    e_s[row, tok], hc_s[row, :], TN, preferred_element_type=F32).astype(BF16)

    enter(0)
    for c in range(nchunk):
        project(0, c)
    enter(1)
    for i in range(nblk + 2):
        enter(i + 2)
        residual(i - 1)
        for c in range(nchunk):
            activate(i, c)
            project(i + 1, c)
        errors(i - 1)
        back_t(i - 2)
        if i < nblk:
            back(i - 2)
        if i == min(3, nblk):
            pl.semaphore_wait(barrier, n - 1)
            for c in cnt_copies:
                c.start()

    @pl.when(me != n)
    def _():
        for c in cnt_copies:
            c.wait()
        cnt_recv[me] = cnt_send[...]
        tot = cnt_recv[0]
        for j in range(1, n):
            tot += cnt_recv[j]
        inv = 1.0 / jnp.maximum(tot.sum(axis=1, keepdims=True), 1.0)
        inv_s[...] = jnp.broadcast_to(inv, (8, LANES))

    my_y, my_x, my_c = me // 4, (me // 2) % 2, me % 2

    def order(s):
        return my_y * s + (1 - my_y) * (nchunk - 1 - s)

    def w2_products(s):
        acc_s[s % 2] = jnp.dot(dzt_s[...], a_s[:, chunk(order(s))], preferred_element_type=F32)

    def w2_scale(s):
        inv0, inv1 = inv_s[0:1, 0:1], inv_s[1:2, 0:1]
        d = acc_s[s % 2]
        tail = 2 * LANES + (model - LANES)
        d = jnp.concatenate([d[:LANES] * inv0, d[LANES:2 * LANES] * inv1,
                             d[2 * LANES:tail] * inv0, d[tail:] * inv1], axis=0)
        send2[chunk(order(s)), :] = d.T.astype(BF16)

    def rows_of(peer):
        return send2.at[pl.ds(pl.multiple_of(peer * rows_out, rows_out), rows_out)]

    out_copies = copies(1, rows_of, recv2.at[me])

    def w2_send(s):
        if s == nchunk - 1:
            for k in (2, 3, 1):
                out_copies[k - 1].start()
            return
        to_x = (1 - my_y) * (1 - s) + my_y * s
        for to_c in range(2):
            peer = (1 - my_y) * 4 + to_x * 2 + to_c
            k = 4 + 2 * ((my_x + to_x) % 2) + (my_c + to_c) % 2
            pltpu.make_async_remote_copy(
                src_ref=rows_of(peer), dst_ref=recv2.at[me], send_sem=send_sem.at[1, k],
                recv_sem=recv_sem.at[1, k], device_id=(peer,), device_id_type=MESH).start()

    for s in range(nchunk + 1):
        @pl.when(me != n + 1 + s)
        def _():
            if s > 0:
                w2_scale(s - 1)
                w2_send(s - 1)
            if s < nchunk:
                w2_products(s)
            if s == nchunk:
                back(nblk - 2)
                back(nblk - 1)

    inv0, inv1 = inv_s[0:1, 0:1], inv_s[1:2, 0:1]

    def copies_in(c):
        return copies(2 + c, lambda peer: send1.at[c, peer], recv1.at[c, me])

    def w1_part(c, carry):
        for i in range(nblk):
            for t in range(2):
                da = jnp.dot(dz_s[t, block(i), :], w2h_s[:, chunk(c)], preferred_element_type=F32)
                for r in range(0, tb, rp):
                    rows = slice(i * tb + r, i * tb + r + rp)
                    if t == 0:
                        p = p_s[rows, chunk(c)]
                        p2 = p * p
                        th = jnp.tanh(p * (2 * C0 + (8 * C0 * C1) * p2))
                        sl = (1.0 + th) * (1.0 + p * ((1.0 - th) * (2 * C0 + (24 * C0 * C1) * p2)))
                        sl_s[r:r + rp, :] = sl
                    else:
                        sl = sl_s[r:r + rp, :]
                    q_s[t, rows, :] = (da[r:r + rp] * sl).astype(BF16)
        d0 = jnp.dot(xt_ref[...], q_s[0], preferred_element_type=F32) * inv0
        d1 = jnp.dot(xt_ref[...], q_s[1], preferred_element_type=F32) * inv1
        for j in range(n):
            r = slice(j * rows_in, (j + 1) * rows_in)
            send1[c, j] = jnp.concatenate([d0[r], d1[r]], axis=0).astype(BF16)
        now = copies_in(c)
        for k in (6, 7, 4, 5, 2, 3, 1):
            now[k - 1].start()
        return carry

    lax.fori_loop(0, nchunk, w1_part, 0)

    for cp in out_copies:
        cp.wait()
    recv2[me] = send2[pl.ds(pl.multiple_of(me * rows_out, rows_out), rows_out), :]
    g2 = recv2[0].astype(F32)
    for j in range(1, n):
        g2 += recv2[j].astype(F32)
    t0, t1, r = g2[:, :LANES], g2[:, LANES:2 * LANES], g2[:, 2 * LANES:]
    r_sw = pltpu.roll(r, LANES // 2, 1)
    low = lax.broadcasted_iota(jnp.int32, (1, LANES), 1) < LANES // 2

    def fold(v):
        s = v[0:8]
        for b in range(1, v.shape[0] // 8):
            s += v[8 * b:8 * b + 8]
        return s

    zero = jnp.zeros((8, LANES), F32)
    rr = fold(r * r)
    m00 = fold(t0 * t0) + jnp.where(low, rr, zero)
    m11 = fold(t1 * t1) + jnp.where(low, zero, rr)
    m01 = fold(t0 * t1) + jnp.where(low, fold(r * r_sw), zero)

    pairs = rows_out // 2
    for t, flat in ((0, flat0), (1, flat1)):
        ta_s[...] = t0 if t == 0 else t1
        tr_s[...] = r if t == 0 else r_sw
        a_e, a_o = ta_s[pl.ds(0, pairs, stride=2), :], ta_s[pl.ds(1, pairs, stride=2), :]
        r_e, r_o = tr_s[pl.ds(0, pairs, stride=2), :], tr_s[pl.ds(1, pairs, stride=2), :]
        a_w = pltpu.roll(a_o, LANES // 2, 1)
        flat[1, pl.ds(0, pairs, stride=3), :] = a_e
        flat[1, pl.ds(1, pairs, stride=3), :] = jnp.where(low, r_e, a_w)
        flat[1, pl.ds(2, pairs, stride=3), :] = jnp.where(low, a_w, pltpu.roll(r_o, LANES // 2, 1))

    wide = hidden // LANES
    for c in range(nchunk):
        for cp in copies_in(c):
            cp.wait()
        recv1[c, me] = send1[c, me]
        g1 = recv1[c, 0].astype(F32)
        for j in range(1, n):
            g1 += recv1[c, j].astype(F32)
        for b in range(fc // LANES):
            u = g1[:rows_in, b * LANES:(b + 1) * LANES]
            v = g1[rows_in:, b * LANES:(b + 1) * LANES]
            m00 += fold(u * u)
            m11 += fold(v * v)
            m01 += fold(u * v)
            flat0[0, pl.ds(c * (fc // LANES) + b, rows_in, stride=wide), :] = u
            flat1[0, pl.ds(c * (fc // LANES) + b, rows_in, stride=wide), :] = v

    row = lax.broadcasted_iota(jnp.int32, (8, LANES), 0)
    m_send[...] = jnp.where(row == 0, m00.sum(axis=0, keepdims=True),
                            jnp.where(row == 1, m01.sum(axis=0, keepdims=True),
                                      jnp.where(row == 2, m11.sum(axis=0, keepdims=True), zero)))
    m_copies = copies(2 + nchunk, lambda peer: m_send, m_recv.at[me])
    for cp in m_copies:
        cp.start()
    saves = [pltpu.make_async_copy(flat0, u0_ref, save_sem.at[0]), pltpu.make_async_copy(flat1, u1_ref, save_sem.at[1])]
    for cp in saves:
        cp.start()
    for cp in m_copies:
        cp.wait()
    m_recv[me] = m_send[...]
    gram = m_recv[0]
    for j in range(1, n):
        gram += m_recv[j]
    gram_ref[...] = gram
    for cp in saves:
        cp.wait()


def finish(u0_ref, u1_ref, gram_ref, alpha_ref, gin_ref, gout_ref):
    gram = jnp.broadcast_to(gram_ref[...].sum(axis=1, keepdims=True), (8, LANES))
    g00, g01, g11 = gram[0:1], gram[1:2], gram[2:3]
    scale = 1.0 / ((g00 + g11) * 0.5)
    b0, b1 = (g00 - g01) * scale, (g01 - g11) * scale
    shift, turn = 0.25 * (b0 + b1), 0.25 * (b1 - b0)
    h = jnp.zeros((1, LANES), F32)
    for _ in range(SOLVER_STEPS):
        h = (h + shift) + turn * jnp.tanh(h)
    ratio = jnp.exp(h + h)
    a0 = 1.0 / (1.0 + ratio)
    a1 = ratio * a0
    alpha_ref[0] = a0[0, 0]
    alpha_ref[1] = a1[0, 0]
    gin_ref[...] = a0 * u0_ref[0] + a1 * u1_ref[0]
    gout_ref[...] = a0 * u0_ref[1] + a1 * u1_ref[1]


def solution(mesh):
    n = mesh.shape["data"]
    tb, rp, fc = 512, 64, 256

    def local_step(x_loc, w_in, w_out, task_heads, lab_loc, mask_loc):
        tokens, model = x_loc.shape
        hidden = w_in.shape[1]
        nchunk = hidden // fc
        piece = model * hidden // n // LANES
        rows_in, rows_out = model // n, hidden // n
        vmem = pl.BlockSpec(memory_space=pltpu.VMEM)
        u0, u1, gram = pl.pallas_call(
            functools.partial(kernel, n, tb, rp, fc),
            out_shape=(jax.ShapeDtypeStruct((2, piece, LANES), F32),
                       jax.ShapeDtypeStruct((2, piece, LANES), F32),
                       jax.ShapeDtypeStruct((8, LANES), F32)),
            in_specs=[vmem] * 6,
            out_specs=(pl.BlockSpec(memory_space=pl.ANY), pl.BlockSpec(memory_space=pl.ANY), vmem),
            scratch_shapes=[
                pltpu.VMEM((tokens, model), BF16),
                pltpu.VMEM((tb, fc), F32),
                pltpu.VMEM((tokens, hidden), BF16),
                pltpu.VMEM((tokens, hidden), F32),
                pltpu.VMEM((2 * SLOT, tokens), BF16),
                pltpu.VMEM((2, tokens, model), BF16),
                pltpu.VMEM((2 * model, tokens), BF16),
                pltpu.VMEM((tokens, model), BF16),
                pltpu.VMEM((2, 2 * model, fc), F32),
                pltpu.VMEM((8, LANES), F32),
                pltpu.VMEM((model, hidden), BF16),
                pltpu.VMEM((model, hidden), BF16),
                pltpu.VMEM((2, tokens, fc), BF16),
                pltpu.VMEM((hidden, model), BF16),
                pltpu.VMEM((2 * SLOT, model), BF16),
                pltpu.VMEM((2 * model, 2 * SLOT), BF16),
                pltpu.VMEM((hidden, 2 * model), BF16),
                pltpu.VMEM((n, rows_out, 2 * model), BF16),
                pltpu.VMEM((nchunk, n, 2 * rows_in, fc), BF16),
                pltpu.VMEM((nchunk, n, 2 * rows_in, fc), BF16),
                pltpu.VMEM((8, LANES), F32),
                pltpu.VMEM((n, 8, LANES), F32),
                pltpu.VMEM((8, LANES), F32),
                pltpu.VMEM((n, 8, LANES), F32),
                pltpu.VMEM((2, piece, LANES), F32),
                pltpu.VMEM((2, piece, LANES), F32),
                pltpu.VMEM((rows_out, LANES), F32),
                pltpu.VMEM((rows_out, LANES), F32),
                pltpu.SemaphoreType.DMA((3 + nchunk, n)),
                pltpu.SemaphoreType.DMA((3 + nchunk, n)),
                pltpu.SemaphoreType.DMA((2,)),
            ],
            compiler_params=pltpu.CompilerParams(
                collective_id=0, has_side_effects=True, vmem_limit_bytes=65000 * 1024),
        )(x_loc.T, w_in, w_out.T, jnp.transpose(task_heads, (2, 0, 1)), lab_loc, mask_loc)
        alpha, g_in, g_out = pl.pallas_call(
            finish,
            out_shape=(jax.ShapeDtypeStruct((2,), F32),
                       jax.ShapeDtypeStruct((piece, LANES), F32),
                       jax.ShapeDtypeStruct((piece, LANES), F32)),
            in_specs=[vmem] * 3,
            out_specs=(pl.BlockSpec(memory_space=pltpu.SMEM), vmem, vmem),
        )(u0, u1, gram)
        return alpha, g_in.reshape(-1), g_out.reshape(-1)

    return jax.shard_map(local_step, mesh=mesh, in_specs=(P("data", None), P(), P(), P(), P(None, "data"), P(None, "data")), out_specs=(P(), P("data"), P("data")), check_vma=False)
```
